8 devices in a mesh: by: 2 (over z, y), bx: 4 (over x, core).
Axes of the slice: x: 2, y: 2, z: 1, core: 2. Of those that a mesh axis runs over, the one named last changes fastest.
Arguments:
- wave_fn: float32 [512, 4, 4, 512], P('bx', None, None, 'by')
- left_env: float32 [512, 4, 512], P('bx')
- mpo_ten: float32 [4, 4, 4, 4], replicated
- right_env: float32 [512, 4, 512], P('by')
Outputs:
- output: float32 [512, 4, 4, 512], P('bx', None, None, 'by')
All inputs are finite; a program needn't handle non-finite values.
Results may differ from the reference program's by a relative error of at most 0.001.
Values sent between devices are 32-bit elements.
A program may use at most 1 GiB of HBM per device.

```python
import jax
import jax.numpy as jnp
from jax import lax

BOND_DIM = 512
PHYS_DIM = 4
MPO_DIM = 4


def setup_inputs(seed: int = 0) -> dict:
    key = jax.random.key(seed)
    k_wave, k_left, k_mpo, k_right = jax.random.split(key, 4)
    wave_fn = jax.random.normal(k_wave, (BOND_DIM, PHYS_DIM, PHYS_DIM, BOND_DIM), jnp.float32)
    left_env = jax.random.normal(k_left, (BOND_DIM, MPO_DIM, BOND_DIM), jnp.float32) * (BOND_DIM ** -0.5)
    mpo_ten = jax.random.normal(k_mpo, (MPO_DIM, PHYS_DIM, PHYS_DIM, MPO_DIM), jnp.float32) * ((MPO_DIM * PHYS_DIM) ** -0.5)
    right_env = jax.random.normal(k_right, (BOND_DIM, MPO_DIM, BOND_DIM), jnp.float32) * ((MPO_DIM * BOND_DIM) ** -0.5)
    return {'wave_fn': wave_fn, 'left_env': left_env, 'mpo_ten': mpo_ten, 'right_env': right_env}


def reference(wave_fn, left_env, mpo_ten, right_env):
    row_block = min(BOND_DIM, 128)
    block_count = BOND_DIM // row_block
    left_blocks = left_env.reshape(block_count, row_block, MPO_DIM, BOND_DIM)

    def one_block(left_rows):
        stage_one = jnp.einsum('auc,cpqf->aupqf', left_rows.astype(jnp.float32), wave_fn.astype(jnp.float32))
        stage_two = jnp.einsum('aupqf,uspv->asvqf', stage_one, mpo_ten.astype(jnp.float32))
        stage_three = jnp.einsum('asvqf,vtqr->astrf', stage_two, mpo_ten.astype(jnp.float32))
        return jnp.einsum('astrf,brf->astb', stage_three, right_env.astype(jnp.float32))

    out_blocks = lax.map(one_block, left_blocks)
    return out_blocks.reshape(BOND_DIM, PHYS_DIM, PHYS_DIM, BOND_DIM)
```

```python
import functools

import jax
import jax.numpy as jnp
from jax import lax
from jax.experimental import pallas as pl
from jax.experimental.pallas import tpu as pltpu
from jax.sharding import PartitionSpec as P

HI = lax.Precision.HIGHEST
F32 = jnp.float32
LANE = 128
T1_PQ = 4
T3_GROUPS = 4
Y_ROWS = 1024
OWN, OTHER = 0, 1


def dot(a, b):
    return jnp.dot(a, b, precision=HI, preferred_element_type=F32)


def kernel(x_ref, l_ref, w_ref, r_ref, y_ref, xg, ln, l2, rn, rt, t1s, t3s, ys, yo, kron, wa, wb, scale, load_sem, env_sem, out_sem, send_sem, recv_sem):
    by = lax.axis_index('by')
    bx = lax.axis_index('bx')
    core = lax.rem(bx, 2)
    chip = bx // 2
    sib = {'by': by, 'bx': bx + 1 - 2 * core}
    xnb = {'by': by, 'bx': lax.rem(bx + 2, 4)}
    ynb = {'by': 1 - by, 'bx': bx}

    loads = []
    for h in range(2):
        for pq in range(16):
            loads.append(pltpu.make_async_copy(
                x_ref.at[:, pq // 4, pq % 4, pl.ds(h * LANE, LANE)],
                xg.at[OWN, h, OWN, core, pq], load_sem.at[h, pq]))
    for cp in loads:
        cp.start()
    env = []
    for half in range(2):
        for k in range(2):
            c0 = ((chip + half) % 2 * 2 + k) * LANE
            env.append(pltpu.make_async_copy(
                l_ref.at[:, :, pl.ds(pl.multiple_of(c0, LANE), LANE)], ln.at[half, k], env_sem.at[half * 2 + k]))
    for half in range(2):
        for h in range(2):
            f0 = ((by + half) % 2 * 2 + h) * LANE
            for r in range(4):
                env.append(pltpu.make_async_copy(
                    r_ref.at[:, r, pl.ds(pl.multiple_of(f0, LANE), LANE)], rn.at[half * 2 + h, r],
                    env_sem.at[4 + (half * 2 + h) * 4 + r]))
    for cp in env:
        cp.start()

    barrier = pltpu.get_barrier_semaphore()
    for d in (sib, xnb, ynb):
        pl.semaphore_signal(barrier, inc=1, device_id=d, device_id_type=pl.DeviceIdType.MESH)
    pl.semaphore_wait(barrier, 3)

    sends = []

    def send(src, dst, k, h, pp, to):
        n = len(sends)
        cp = pltpu.make_async_remote_copy(
            src_ref=xg.at[src[0], h, src[1], k, pl.ds(pp * 8, 8)],
            dst_ref=xg.at[dst[0], h, dst[1], k, pl.ds(pp * 8, 8)],
            send_sem=send_sem.at[n],
            recv_sem=recv_sem.at[dst[0], h, dst[1], k, pp],
            device_id=to, device_id_type=pl.DeviceIdType.MESH)
        cp.start()
        sends.append(cp)

    def arrived(slot, k, h, pp):
        ref = xg.at[slot[0], h, slot[1], k, pl.ds(pp * 8, 8)]
        pltpu.make_async_copy(ref, ref, recv_sem.at[slot[0], h, slot[1], k, pp]).wait()

    me, x_slot, y_slot, d_slot = (OWN, OWN), (OWN, OTHER), (OTHER, OWN), (OTHER, OTHER)
    for h in range(2):
        for pp in range(2):
            for cp in loads[h * 16 + pp * 8:h * 16 + pp * 8 + 8]:
                cp.wait()
            send(me, x_slot, core, h, pp, xnb)
            send(me, y_slot, core, h, pp, ynb)
            send(me, me, core, h, pp, sib)

    def relay(h, pp):
        arrived(x_slot, core, h, pp)
        send(x_slot, x_slot, core, h, pp, sib)
        if pp == 0:
            send(x_slot, d_slot, core, h, pp, ynb)
        arrived(y_slot, core, h, pp)
        send(y_slot, y_slot, core, h, pp, sib)
        if pp == 1:
            send(y_slot, d_slot, core, h, pp, xnb)

    def relay_diag(h):
        for pp in range(2):
            arrived(d_slot, core, h, pp)
            send(d_slot, d_slot, core, h, pp, sib)

    for cp in env[:4]:
        cp.wait()
    for half in range(2):
        for k in range(2):
            l2[half, :, k * LANE:(k + 1) * LANE] = ln[half, k].reshape(512, LANE)
    wa[...] = jnp.zeros_like(wa)
    wb[...] = jnp.zeros_like(wb)
    lane8 = lax.broadcasted_iota(jnp.int32, (8, LANE), 1)
    row8 = lax.broadcasted_iota(jnp.int32, (8, LANE), 0)
    lane16 = lax.broadcasted_iota(jnp.int32, (16, LANE), 1)
    row16 = lax.broadcasted_iota(jnp.int32, (16, LANE), 0)

    def fill(i, carry):
        va, vb = carry
        i0, i1, i2 = i // 16, i // 4 % 4, i % 4
        for i3 in range(4):
            val = w_ref[i0, i1, i2, i3]
            va = jnp.where((row8 == i1) & (lane8 == i0 * 16 + i2 * 4 + i3), val, va)
            vb = jnp.where((row16 == i3 * 4 + i1) & (lane16 == i0 * 4 + i2), val, vb)
        return va, vb

    va, vb = lax.fori_loop(0, 64, fill, (jnp.zeros((8, LANE), F32), jnp.zeros((16, LANE), F32)))
    top = jnp.max(jnp.max(jnp.abs(va), axis=1, keepdims=True), axis=0, keepdims=True)
    scale[...] = jnp.broadcast_to(top, scale.shape)
    wa[...] = va / scale[...]
    wb[...] = vb / jnp.broadcast_to(top, (16, LANE))

    row = lax.broadcasted_iota(jnp.int32, (256, LANE), 0)
    a_mat = jnp.zeros((256, LANE), F32)
    for s in range(4):
        a_mat = jnp.where(row // 4 % 4 == s, wa[s:s + 1, :], a_mat)
    c_mat = jnp.zeros((256, LANE), F32)
    for rt_ in range(16):
        c_mat = jnp.where((row // 64) * 4 + row % 4 == rt_, wb[rt_:rt_ + 1, :], c_mat)
    col = lax.broadcasted_iota(jnp.int32, (LANE, 256), 1)
    pick = lax.broadcasted_iota(jnp.int32, (LANE, 256), 0)
    total = jnp.zeros((256, 256), F32)
    for v in range(4):
        left = dot(a_mat, jnp.where(pick == col % 4 * 16 + col // 64 * 4 + v, 1.0, 0.0).astype(F32))
        right = dot(c_mat, jnp.where(pick == v * 4 + col // 16 % 4, 1.0, 0.0).astype(F32))
        total = total + left * right
    krow = lax.broadcasted_iota(jnp.int32, (256, 256), 0)
    kcol = lax.broadcasted_iota(jnp.int32, (256, 256), 1)
    kron[...] = jnp.where(krow // 16 % 4 == kcol // 4 % 4, total, 0.0)
    for cp in env[4:]:
        cp.wait()
    for fc in range(4):
        for r in range(4):
            rt[fc, r * LANE:(r + 1) * LANE, :] = rn[fc, r].T

    def stage1(slot, h, pp, first):
        fh, ch = slot
        buf = fh * 2 + h

        def body(j, _):
            pq = pp * 8 + T1_PQ * j
            xs = jnp.concatenate([
                jnp.concatenate([xg[fh, h, ch, k, pq + n] for n in range(T1_PQ)], axis=1) for k in range(2)], axis=0)
            t = dot(l2[ch], xs)
            for ab in range(2):
                for n in range(T1_PQ):
                    dst = (buf, slice(None), pl.ds(pl.multiple_of((pq + n) * 16, 16), 16), slice(ab * LANE, (ab + 1) * LANE))
                    part = t[ab * 256:(ab + 1) * 256, n * LANE:(n + 1) * LANE].reshape(16, 16, LANE)
                    t1s[dst] = part if first else t1s[dst] + part
            return 0

        lax.fori_loop(0, 8 // T1_PQ, body, 0)

    def stage23(fh, h, first, final):
        buf = fh * 2 + h
        sc = scale[0:1, 0:1]

        def body(i, _):
            ts = jnp.concatenate([t1s[buf, i * T3_GROUPS + g] for g in range(T3_GROUPS)], axis=1)
            t = dot(kron[...], ts * sc) * sc
            for g in range(T3_GROUPS):
                for ab in range(2):
                    lanes = slice(g * 256 + ab * LANE, g * 256 + (ab + 1) * LANE)
                    rows = pl.ds(pl.multiple_of(ab * 1024 + (i * T3_GROUPS + g) * 64, 64), 64)
                    for r in range(4):
                        t3s[rows, r * LANE:(r + 1) * LANE] = t[r * 64:(r + 1) * 64, lanes]
            return 0

        lax.fori_loop(0, 16 // T3_GROUPS, body, 0)

        def last(i, _):
            rows = pl.ds(pl.multiple_of(i * Y_ROWS, Y_ROWS), Y_ROWS)
            t = dot(t3s[rows, :], rt[buf])
            for b in range(2):
                part = t[:, b * LANE:(b + 1) * LANE]
                if not first:
                    part = ys[b, rows, :] + part
                if final:
                    yo[b, pl.ds(i * (Y_ROWS // 16), Y_ROWS // 16)] = part.reshape(Y_ROWS // 16, 4, 4, LANE)
                    out_copy(b, i).start()
                else:
                    ys[b, rows, :] = part
            return 0

        lax.fori_loop(0, 2048 // Y_ROWS, last, 0)

    def out_copy(b, i):
        part = pl.ds(i * (Y_ROWS // 16), Y_ROWS // 16)
        return pltpu.make_async_copy(yo.at[b, part], y_ref.at[part, :, :, pl.ds(b * LANE, LANE)], out_sem.at[b, i])

    other_core = 1 - core
    for h in range(2):
        for pp in range(2):
            arrived(me, other_core, h, pp)
            stage1(me, h, pp, True)
    for h in range(2):
        for pp in range(2):
            relay(h, pp)
            arrived(x_slot, other_core, h, pp)
            stage1(x_slot, h, pp, False)
            arrived(y_slot, other_core, h, pp)
            stage1(y_slot, h, pp, True)
        stage23(OWN, h, h == 0, False)
    for h in range(2):
        relay_diag(h)
        for pp in range(2):
            arrived(d_slot, other_core, h, pp)
            stage1(d_slot, h, pp, False)
        stage23(OTHER, h, False, h == 1)

    for i in range(2048 // Y_ROWS):
        for b in range(2):
            out_copy(b, i).wait()
    for cp in sends:
        cp.wait_send()


def solution(mesh):
    def local_apply(x, left, mpo, right):
        any_spec = pl.BlockSpec(memory_space=pl.ANY)
        return pl.pallas_call(
            kernel,
            out_shape=jax.ShapeDtypeStruct((128, 4, 4, 256), F32),
            in_specs=[any_spec, any_spec, pl.BlockSpec(memory_space=pltpu.SMEM), any_spec],
            out_specs=any_spec,
            scratch_shapes=[
                pltpu.VMEM((2, 2, 2, 2, 16, 128, LANE), F32),
                pltpu.VMEM((2, 2, 128, 4, LANE), F32),
                pltpu.VMEM((2, 512, 256), F32),
                pltpu.VMEM((4, 4, 256, LANE), F32),
                pltpu.VMEM((4, 512, 256), F32),
                pltpu.VMEM((4, 16, 256, 256), F32),
                pltpu.VMEM((2048, 512), F32),
                pltpu.VMEM((2, 2048, LANE), F32),
                pltpu.VMEM((2, 128, 4, 4, LANE), F32),
                pltpu.VMEM((256, 256), F32),
                pltpu.VMEM((8, LANE), F32),
                pltpu.VMEM((16, LANE), F32),
                pltpu.VMEM((8, LANE), F32),
                pltpu.SemaphoreType.DMA((2, 16)),
                pltpu.SemaphoreType.DMA((20,)),
                pltpu.SemaphoreType.DMA((2, 2048 // Y_ROWS)),
                pltpu.SemaphoreType.DMA((28,)),
                pltpu.SemaphoreType.DMA((2, 2, 2, 2, 2)),
            ],
            compiler_params=pltpu.CompilerParams(collective_id=0, has_side_effects=True, vmem_limit_bytes=62 * 2**20),
            name='two_site',
        )(x, left, mpo, right)

    return jax.shard_map(local_apply, mesh=mesh, in_specs=(P('bx', None, None, 'by'), P('bx', None, None), P(), P('by', None, None)), out_specs=P('bx', None, None, 'by'), check_vma=False)
```

```python
import functools

import jax
import jax.numpy as jnp
from jax import lax
from jax.experimental import pallas as pl
from jax.experimental.pallas import tpu as pltpu
from jax.sharding import PartitionSpec as P

HI = lax.Precision.HIGHEST
F32 = jnp.float32
LANE = 128
T3_GROUPS = 8
Y_ROWS = 1024
OWN, OTHER = 0, 1


def dot(a, b):
    return jnp.dot(a, b, precision=HI, preferred_element_type=F32)


def kernel(x_ref, l_ref, w_ref, r_ref, y_ref, xg, ln, l2, rn, rt, t1s, t3s, ys, yo, kron, wa, wb, scale, load_sem, env_sem, out_sem, send_sem, recv_sem):
    by = lax.axis_index('by')
    bx = lax.axis_index('bx')
    core = lax.rem(bx, 2)
    chip = bx // 2
    sib = {'by': by, 'bx': bx + 1 - 2 * core}
    xnb = {'by': by, 'bx': lax.rem(bx + 2, 4)}
    ynb = {'by': 1 - by, 'bx': bx}

    loads = []
    for h in range(2):
        for pq in range(16):
            loads.append(pltpu.make_async_copy(
                x_ref.at[:, pq // 4, pq % 4, pl.ds(h * LANE, LANE)],
                xg.at[OWN, h, OWN, core, pq], load_sem.at[h, pq]))
    for cp in loads:
        cp.start()
    env = []
    for half in range(2):
        for k in range(2):
            c0 = ((chip + half) % 2 * 2 + k) * LANE
            env.append(pltpu.make_async_copy(
                l_ref.at[:, :, pl.ds(pl.multiple_of(c0, LANE), LANE)], ln.at[half, k], env_sem.at[half * 2 + k]))
    for half in range(2):
        for h in range(2):
            f0 = ((by + half) % 2 * 2 + h) * LANE
            for r in range(4):
                env.append(pltpu.make_async_copy(
                    r_ref.at[:, r, pl.ds(pl.multiple_of(f0, LANE), LANE)], rn.at[half * 2 + h, r],
                    env_sem.at[4 + (half * 2 + h) * 4 + r]))
    for cp in env:
        cp.start()

    barrier = pltpu.get_barrier_semaphore()
    for d in (sib, xnb, ynb):
        pl.semaphore_signal(barrier, inc=1, device_id=d, device_id_type=pl.DeviceIdType.MESH)
    pl.semaphore_wait(barrier, 3)

    def send(kind, h, pp):
        fh, ch = ((0, 0), (0, 0), (0, 0), (0, 1), (1, 0), (1, 1), (pp, 1 - pp))[kind]
        dh, dc = ((0, 1), (1, 0), (0, 0), (0, 1), (1, 0), (1, 1), (1, 1))[kind]
        to = (xnb, ynb, sib, sib, sib, sib, {'by': lax.rem(by + 1 - pp, 2), 'bx': lax.rem(bx + 2 * pp, 4)})[kind]
        return pltpu.make_async_remote_copy(
            src_ref=xg.at[fh, h, ch, core, pl.ds(pp * 8, 8)],
            dst_ref=xg.at[dh, h, dc, core, pl.ds(pp * 8, 8)],
            send_sem=send_sem.at[kind, h, pp],
            recv_sem=recv_sem.at[dh, h, dc, core, pp],
            device_id=to, device_id_type=pl.DeviceIdType.MESH)

    def arrived(fh, ch, k, h, pp):
        ref = xg.at[fh, h, ch, k, pl.ds(pp * 8, 8)]
        pltpu.make_async_copy(ref, ref, recv_sem.at[fh, h, ch, k, pp]).wait()

    for h in range(2):
        for pp in range(2):
            for cp in loads[h * 16 + pp * 8:h * 16 + pp * 8 + 8]:
                cp.wait()
            for kind in range(3):
                send(kind, h, pp).start()

    def relay(h, pp):
        arrived(OWN, OTHER, core, h, pp)
        send(3, h, pp).start()
        arrived(OTHER, OWN, core, h, pp)
        send(4, h, pp).start()
        send(6, h, pp).start()

    def relay_diag(h):
        for pp in range(2):
            arrived(OTHER, OTHER, core, h, pp)
            send(5, h, pp).start()

    for cp in env[:4]:
        cp.wait()
    for half in range(2):
        for k in range(2):
            l2[half, :, k * LANE:(k + 1) * LANE] = ln[half, k].reshape(512, LANE)
    wa[...] = jnp.zeros_like(wa)
    wb[...] = jnp.zeros_like(wb)
    lane8 = lax.broadcasted_iota(jnp.int32, (8, LANE), 1)
    row8 = lax.broadcasted_iota(jnp.int32, (8, LANE), 0)
    lane16 = lax.broadcasted_iota(jnp.int32, (16, LANE), 1)
    row16 = lax.broadcasted_iota(jnp.int32, (16, LANE), 0)

    def fill(i, carry):
        va, vb = carry
        i0, i1, i2 = i // 16, i // 4 % 4, i % 4
        for i3 in range(4):
            val = w_ref[i0, i1, i2, i3]
            va = jnp.where((row8 == i1) & (lane8 == i0 * 16 + i2 * 4 + i3), val, va)
            vb = jnp.where((row16 == i3 * 4 + i1) & (lane16 == i0 * 4 + i2), val, vb)
        return va, vb

    va, vb = lax.fori_loop(0, 64, fill, (jnp.zeros((8, LANE), F32), jnp.zeros((16, LANE), F32)))
    top = jnp.max(jnp.max(jnp.abs(va), axis=1, keepdims=True), axis=0, keepdims=True)
    scale[...] = jnp.broadcast_to(top, scale.shape)
    wa[...] = va / scale[...]
    wb[...] = vb / jnp.broadcast_to(top, (16, LANE))

    row = lax.broadcasted_iota(jnp.int32, (256, LANE), 0)
    a_mat = jnp.zeros((256, LANE), F32)
    for s in range(4):
        a_mat = jnp.where(row // 4 % 4 == s, wa[s:s + 1, :], a_mat)
    c_mat = jnp.zeros((256, LANE), F32)
    for rt_ in range(16):
        c_mat = jnp.where((row // 64) * 4 + row % 4 == rt_, wb[rt_:rt_ + 1, :], c_mat)
    col = lax.broadcasted_iota(jnp.int32, (LANE, 256), 1)
    pick = lax.broadcasted_iota(jnp.int32, (LANE, 256), 0)
    total = jnp.zeros((256, 256), F32)
    for v in range(4):
        left = dot(a_mat, jnp.where(pick == col % 4 * 16 + col // 64 * 4 + v, 1.0, 0.0).astype(F32))
        right = dot(c_mat, jnp.where(pick == v * 4 + col // 16 % 4, 1.0, 0.0).astype(F32))
        total = total + left * right
    krow = lax.broadcasted_iota(jnp.int32, (256, 256), 0)
    kcol = lax.broadcasted_iota(jnp.int32, (256, 256), 1)
    kron[...] = jnp.where(krow // 16 % 4 == kcol // 4 % 4, total, 0.0)
    for cp in env[4:]:
        cp.wait()
    for fc in range(4):
        for r in range(4):
            rt[fc, r * LANE:(r + 1) * LANE, :] = rn[fc, r].T

    def stage1(fh, ch, h, pp, first):
        buf = fh * 2 + h
        xs = jnp.concatenate([
            jnp.concatenate([xg[fh, h, ch, k, pp * 8 + n] for n in range(8)], axis=1) for k in range(2)], axis=0)
        t = dot(l2[ch], xs)
        for n in range(8):
            row0 = (pp * 8 + n) * 16
            if not isinstance(pp, int):
                row0 = pl.multiple_of(row0, 16)
            for ab in range(2):
                dst = (buf, slice(None), pl.ds(row0, 16), slice(ab * LANE, (ab + 1) * LANE))
                part = t[ab * 256:(ab + 1) * 256, n * LANE:(n + 1) * LANE].reshape(16, 16, LANE)
                t1s[dst] = part if first else t1s[dst] + part

    def stage2(fh, h):
        buf = fh * 2 + h
        sc = scale[0:1, 0:1]

        def body(i, _):
            for g in range(T3_GROUPS):
                t = dot(kron[...], t1s[buf, i * T3_GROUPS + g] * sc) * sc
                for ab in range(2):
                    rows = pl.ds(pl.multiple_of(ab * 1024 + (i * T3_GROUPS + g) * 64, 64), 64)
                    for r in range(4):
                        t3s[rows, r * LANE:(r + 1) * LANE] = t[r * 64:(r + 1) * 64, ab * LANE:(ab + 1) * LANE]
            return 0

        lax.fori_loop(0, 16 // T3_GROUPS, body, 0)

    def stage3(fh, h, between=None, final=False):
        buf = fh * 2 + h

        def body(i, _):
            rows = pl.ds(pl.multiple_of(i * Y_ROWS, Y_ROWS), Y_ROWS)
            t = dot(t3s[rows, :], rt[buf])
            for b in range(2):
                part = t[:, b * LANE:(b + 1) * LANE]
                if fh == 0:
                    part = part + jnp.where(h == 0, 0.0, ys[b, rows, :])
                else:
                    part = part + ys[b, rows, :]
                if final:
                    yo[b, pl.ds(i * (Y_ROWS // 16), Y_ROWS // 16)] = part.reshape(Y_ROWS // 16, 4, 4, LANE)
                    out_copy(b, i).start()
                else:
                    ys[b, rows, :] = part
            if between is not None:
                pl.when(i == 0)(between)
            return 0

        lax.fori_loop(0, 2048 // Y_ROWS, body, 0)

    def out_copy(b, i):
        part = pl.ds(i * (Y_ROWS // 16), Y_ROWS // 16)
        return pltpu.make_async_copy(yo.at[b, part], y_ref.at[part, :, :, pl.ds(b * LANE, LANE)], out_sem.at[b, i])

    other_core = 1 - core

    def own_chunk(h, _):
        for pp in range(2):
            arrived(OWN, OWN, other_core, h, pp)
        for pp in range(2):
            stage1(OWN, OWN, h, pp, True)
        return 0

    lax.fori_loop(0, 2, own_chunk, 0)

    def direct_unit(s, _):
        h, pp = s // 2, s % 2
        relay(h, pp)
        arrived(OWN, OTHER, other_core, h, pp)
        arrived(OTHER, OWN, other_core, h, pp)
        stage1(OWN, OTHER, h, pp, False)
        stage1(OTHER, OWN, h, pp, True)

        @pl.when(pp == 1)
        def _():
            stage2(OWN, h)
            stage3(OWN, h, lambda: pl.when(h == 1)(lambda: relay_diag(0)))

        return 0

    lax.fori_loop(0, 4, direct_unit, 0)

    def diagonal(h):
        for pp in range(2):
            arrived(OTHER, OTHER, other_core, h, pp)
        for pp in range(2):
            stage1(OTHER, OTHER, h, pp, False)
        stage2(OTHER, h)

    diagonal(0)
    stage3(OTHER, 0, lambda: relay_diag(1))
    diagonal(1)
    stage3(OTHER, 1, final=True)
    for i in range(2048 // Y_ROWS):
        for b in range(2):
            out_copy(b, i).wait()
    for kind in range(7):
        for h in range(2):
            for pp in range(2):
                send(kind, h, pp).wait_send()


def solution(mesh):
    def local_apply(x, left, mpo, right):
        any_spec = pl.BlockSpec(memory_space=pl.ANY)
        return pl.pallas_call(
            kernel,
            out_shape=jax.ShapeDtypeStruct((128, 4, 4, 256), F32),
            in_specs=[any_spec, any_spec, pl.BlockSpec(memory_space=pltpu.SMEM), any_spec],
            out_specs=any_spec,
            scratch_shapes=[
                pltpu.VMEM((2, 2, 2, 2, 16, 128, LANE), F32),
                pltpu.VMEM((2, 2, 128, 4, LANE), F32),
                pltpu.VMEM((2, 512, 256), F32),
                pltpu.VMEM((4, 4, 256, LANE), F32),
                pltpu.VMEM((4, 512, 256), F32),
                pltpu.VMEM((4, 16, 256, 256), F32),
                pltpu.VMEM((2048, 512), F32),
                pltpu.VMEM((2, 2048, LANE), F32),
                pltpu.VMEM((2, 128, 4, 4, LANE), F32),
                pltpu.VMEM((256, 256), F32),
                pltpu.VMEM((8, LANE), F32),
                pltpu.VMEM((16, LANE), F32),
                pltpu.VMEM((8, LANE), F32),
                pltpu.SemaphoreType.DMA((2, 16)),
                pltpu.SemaphoreType.DMA((20,)),
                pltpu.SemaphoreType.DMA((2, 2048 // Y_ROWS)),
                pltpu.SemaphoreType.DMA((7, 2, 2)),
                pltpu.SemaphoreType.DMA((2, 2, 2, 2, 2)),
            ],
            compiler_params=pltpu.CompilerParams(collective_id=0, has_side_effects=True, vmem_limit_bytes=62 * 2**20),
            name='two_site',
        )(x, left, mpo, right)

    return jax.shard_map(local_apply, mesh=mesh, in_specs=(P('bx', None, None, 'by'), P('bx', None, None), P(), P('by', None, None)), out_specs=P('bx', None, None, 'by'), check_vma=False)
```

```python
import functools

import jax
import jax.numpy as jnp
from jax import lax
from jax.experimental import pallas as pl
from jax.experimental.pallas import tpu as pltpu
from jax.sharding import PartitionSpec as P

HI = lax.Precision.HIGHEST
F32 = jnp.float32
LANE = 128
HALF = 64
GROUPS = 8
OWN, OTHER = 0, 1


def dot(a, b):
    return jnp.dot(a, b, precision=HI, preferred_element_type=F32)


def kernel(x_ref, l_ref, w_ref, r_ref, y_ref, xg, ln, l2, rt, t1r, t1g, t3s, ys, yo, kron, wa, wb, scale, load_sem, env_sem, out_sem, send_sem, recv_sem):
    by = lax.axis_index('by')
    bx = lax.axis_index('bx')
    core = lax.rem(bx, 2)
    chip = bx // 2
    sib = {'by': by, 'bx': bx + 1 - 2 * core}
    xnb = {'by': by, 'bx': lax.rem(bx + 2, 4)}
    ynb = {'by': 1 - by, 'bx': bx}

    def load(h, pq):
        i = h * 16 + pq
        return pltpu.make_async_copy(
            x_ref.at[:, pq // 4, pq % 4, pl.ds(h * LANE, LANE)],
            t1r.at[7, pl.ds(i // 8 * LANE, LANE), pl.ds(i % 8 * LANE, LANE)], load_sem.at[h, pq])

    for h in range(2):
        for pq in range(16):
            load(h, pq).start()
    env = []
    for half in range(2):
        for k in range(2):
            c0 = ((chip + half) % 2 * 2 + k) * LANE
            env.append(pltpu.make_async_copy(
                l_ref.at[:, :, pl.ds(pl.multiple_of(c0, LANE), LANE)], ln.at[half, k], env_sem.at[half * 2 + k]))
    for half in range(2):
        for h in range(2):
            f0 = ((by + half) % 2 * 2 + h) * LANE
            for r in range(4):
                env.append(pltpu.make_async_copy(
                    r_ref.at[:, r, pl.ds(pl.multiple_of(f0, LANE), LANE)],
                    t1r.at[6, pl.ds(half * 256, 256), pl.ds((h * 4 + r) * LANE, LANE)],
                    env_sem.at[4 + (half * 2 + h) * 4 + r]))
    for cp in env:
        cp.start()

    barrier = pltpu.get_barrier_semaphore()
    for d in (sib, xnb, ynb):
        pl.semaphore_signal(barrier, inc=1, device_id=d, device_id_type=pl.DeviceIdType.MESH)
    pl.semaphore_wait(barrier, 3)

    def send(kind, g):
        fh, ch = ((0, 0), (0, 0), (0, 0), (0, 1), (1, 0), (1, 1), (1, 1), (0, 1), (1, 0))[kind]
        dh, dc = ((0, 1), (1, 0), (0, 0), (0, 1), (1, 0), (1, 1), (1, 1), (1, 1), (1, 1))[kind]
        to = (xnb, ynb, sib, sib, sib, sib, sib, ynb, xnb)[kind]
        part = pl.ds(*((0, 8), (0, 8), (0, 8), (0, 8), (0, 8), (0, 4), (4, 4), (0, 4), (4, 4))[kind])
        return pltpu.make_async_remote_copy(
            src_ref=xg.at[fh, g, ch, core, part],
            dst_ref=xg.at[dh, g, dc, core, part],
            send_sem=send_sem.at[kind, g],
            recv_sem=recv_sem.at[dh, g, dc, core, int(kind in (6, 8))],
            device_id=to, device_id_type=pl.DeviceIdType.MESH)

    def arrived(fh, ch, k, g, half=None):
        part = pl.ds(0, 8) if half is None else pl.ds(4 * half, 4)
        ref = xg.at[fh, g, ch, k, part]
        pltpu.make_async_copy(ref, ref, recv_sem.at[fh, g, ch, k, 0 if half is None else half]).wait()

    low = lax.broadcasted_iota(jnp.int32, (LANE, LANE), 1) < HALF

    def swap(v0, v1):
        m = low[:v0.shape[0]]
        return jnp.where(m, v0, pltpu.roll(v1, HALF, 1)), jnp.where(m, pltpu.roll(v0, HALF, 1), v1)

    def split(h):
        for n in range(8):
            v = []
            for pq in (2 * n, 2 * n + 1):
                i = h * 16 + pq
                load(h, pq).wait()
                v.append(t1r[7, i // 8 * LANE:(i // 8 + 1) * LANE, i % 8 * LANE:(i % 8 + 1) * LANE])
            xg[OWN, 2 * h, OWN, core, n], xg[OWN, 2 * h + 1, OWN, core, n] = swap(*v)

    for h in range(2):
        split(h)
        for g in (2 * h, 2 * h + 1):
            for kind in range(3):
                send(kind, g).start()

    def relay(g):
        arrived(OWN, OTHER, core, g)
        send(3, g).start()
        send(7, g).start()
        arrived(OTHER, OWN, core, g)
        send(4, g).start()
        send(8, g).start()

    def relay_diag(g):
        for half in range(2):
            arrived(OTHER, OTHER, core, g, half)
            send(5 + half, g).start()

    for cp in env[:4]:
        cp.wait()
    for half in range(2):
        for k in range(2):
            l2[half, :, k * LANE:(k + 1) * LANE] = ln[half, k].reshape(512, LANE)
    wa[...] = jnp.zeros_like(wa)
    wb[...] = jnp.zeros_like(wb)
    lane8 = lax.broadcasted_iota(jnp.int32, (8, LANE), 1)
    row8 = lax.broadcasted_iota(jnp.int32, (8, LANE), 0)
    lane16 = lax.broadcasted_iota(jnp.int32, (16, LANE), 1)
    row16 = lax.broadcasted_iota(jnp.int32, (16, LANE), 0)

    def fill(i, carry):
        va, vb = carry
        i0, i1, i2 = i // 16, i // 4 % 4, i % 4
        for i3 in range(4):
            val = w_ref[i0, i1, i2, i3]
            va = jnp.where((row8 == i1) & (lane8 == i0 * 16 + i2 * 4 + i3), val, va)
            vb = jnp.where((row16 == i3 * 4 + i1) & (lane16 == i0 * 4 + i2), val, vb)
        return va, vb

    va, vb = lax.fori_loop(0, 64, fill, (jnp.zeros((8, LANE), F32), jnp.zeros((16, LANE), F32)))
    top = jnp.max(jnp.max(jnp.abs(va), axis=1, keepdims=True), axis=0, keepdims=True)
    scale[...] = jnp.broadcast_to(top, scale.shape)
    wa[...] = va / scale[...]
    wb[...] = vb / jnp.broadcast_to(top, (16, LANE))

    row = lax.broadcasted_iota(jnp.int32, (256, LANE), 0)
    a_mat = jnp.zeros((256, LANE), F32)
    for s in range(4):
        a_mat = jnp.where(row // 4 % 4 == s, wa[s:s + 1, :], a_mat)
    c_mat = jnp.zeros((256, LANE), F32)
    for rt_ in range(16):
        c_mat = jnp.where((row // 64) * 4 + row % 4 == rt_, wb[rt_:rt_ + 1, :], c_mat)
    col = lax.broadcasted_iota(jnp.int32, (LANE, 256), 1)
    pick = lax.broadcasted_iota(jnp.int32, (LANE, 256), 0)
    total = jnp.zeros((256, 256), F32)
    for v in range(4):
        left = dot(a_mat, jnp.where(pick == col % 4 * 16 + col // 64 * 4 + v, 1.0, 0.0).astype(F32))
        right = dot(c_mat, jnp.where(pick == v * 4 + col // 16 % 4, 1.0, 0.0).astype(F32))
        total = total + left * right
    krow = lax.broadcasted_iota(jnp.int32, (256, 256), 0)
    kcol = lax.broadcasted_iota(jnp.int32, (256, 256), 1)
    kron[...] = jnp.where(krow // 16 % 4 == kcol // 4 % 4, total, 0.0)
    for cp in env[4:]:
        cp.wait()
    for fc in range(4):
        for r in range(4):
            t = t1r[6, fc // 2 * 256:(fc // 2 + 1) * 256, (fc % 2 * 4 + r) * LANE:(fc % 2 * 4 + r + 1) * LANE].T
            rt[fc * 2, r * HALF:(r + 1) * HALF, :] = t[:HALF]
            rt[fc * 2 + 1, r * HALF:(r + 1) * HALF, :] = t[HALF:]

    def stage1(fh, ch, g, first):
        xs = jnp.concatenate([
            jnp.concatenate([xg[fh, g, ch, k, n] for n in range(8)], axis=1) for k in range(2)], axis=0)
        t = dot(l2[ch], xs)
        if first:
            t1r[fh * 4 + g] = t
            return
        for n in range(8):
            lanes = slice(n * LANE, (n + 1) * LANE)
            for m in range(2):
                v = [t[ab * LANE:(ab + 1) * LANE, lanes] + t1r[fh * 4 + g, ab * LANE:(ab + 1) * LANE, lanes] for ab in (2 * m, 2 * m + 1)]
                for qb, w in enumerate(swap(*v)):
                    t1g[:, (2 * n + qb) * 16:(2 * n + qb + 1) * 16, m * LANE:(m + 1) * LANE] = w.reshape(GROUPS, 16, LANE)

    def stage2(g):
        sc = scale[0:1, 0:1]

        def body(_, c):
            for i in range(GROUPS):
                t = dot(kron[...], t1g[i] * sc) * sc
                for rp in range(2):
                    for m in range(2):
                        v = [t[r * HALF:(r + 1) * HALF, m * LANE:(m + 1) * LANE] for r in (2 * rp, 2 * rp + 1)]
                        for n, w in enumerate(swap(*v)):
                            row0 = (2 * m + n) * 512 + i * 64
                            t3s[row0:row0 + 64, rp * LANE:(rp + 1) * LANE] = w
            return c

        lax.fori_loop(g, g + 1, body, 0)

    def stage3(fh, g, final=False):
        def body(_, c):
            part = dot(t3s[...], rt[fh * 4 + g])
            for b in range(2):
                v = part[:, b * LANE:(b + 1) * LANE]
                v = v + (jnp.where(g == 0, 0.0, ys[b]) if fh == 0 else ys[b])
                if final:
                    yo[b] = v.reshape(128, 4, 4, LANE)
                else:
                    ys[b] = v
            return c

        lax.fori_loop(g, g + 1, body, 0)

    other_core = 1 - core

    def own(i, _):
        for j in range(2):
            arrived(OWN, OWN, other_core, 2 * i + j)
        for j in range(2):
            stage1(OWN, OWN, 2 * i + j, True)
        return 0

    lax.fori_loop(0, 2, own, 0)

    def direct(g, _):
        relay(g)
        arrived(OWN, OTHER, other_core, g)
        arrived(OTHER, OWN, other_core, g)
        stage1(OWN, OTHER, g, False)
        stage1(OTHER, OWN, g, True)
        stage2(g)
        pl.when(g == 3)(lambda: relay_diag(0))
        stage3(OWN, g)
        return 0

    lax.fori_loop(0, 4, direct, 0)

    def diagonal(g, _):
        for half in range(2):
            arrived(OTHER, OTHER, other_core, g, half)
        stage1(OTHER, OTHER, g, False)
        stage2(g)
        pl.when(g < 3)(lambda: relay_diag(g + 1))
        pl.when(g < 3)(lambda: stage3(OTHER, g))
        pl.when(g == 3)(lambda: stage3(OTHER, g, True))
        return 0

    lax.fori_loop(0, 4, diagonal, 0)

    outs = [pltpu.make_async_copy(yo.at[b], y_ref.at[:, :, :, pl.ds(b * LANE, LANE)], out_sem.at[b]) for b in range(2)]
    for cp in outs:
        cp.start()
    for cp in outs:
        cp.wait()
    for kind in range(9):
        for g in range(4):
            send(kind, g).wait_send()


def solution(mesh):
    def local_apply(x, left, mpo, right):
        any_spec = pl.BlockSpec(memory_space=pl.ANY)
        return pl.pallas_call(
            kernel,
            out_shape=jax.ShapeDtypeStruct((128, 4, 4, 256), F32),
            in_specs=[any_spec, any_spec, pl.BlockSpec(memory_space=pltpu.SMEM), any_spec],
            out_specs=any_spec,
            scratch_shapes=[
                pltpu.VMEM((2, 4, 2, 2, 8, 128, LANE), F32),
                pltpu.VMEM((2, 2, 128, 4, LANE), F32),
                pltpu.VMEM((2, 512, 256), F32),
                pltpu.VMEM((8, 256, 256), F32),
                pltpu.VMEM((8, 512, 1024), F32),
                pltpu.VMEM((GROUPS, 256, 256), F32),
                pltpu.VMEM((2048, 256), F32),
                pltpu.VMEM((2, 2048, LANE), F32),
                pltpu.VMEM((2, 128, 4, 4, LANE), F32),
                pltpu.VMEM((256, 256), F32),
                pltpu.VMEM((8, LANE), F32),
                pltpu.VMEM((16, LANE), F32),
                pltpu.VMEM((8, LANE), F32),
                pltpu.SemaphoreType.DMA((2, 16)),
                pltpu.SemaphoreType.DMA((20,)),
                pltpu.SemaphoreType.DMA((2,)),
                pltpu.SemaphoreType.DMA((9, 4)),
                pltpu.SemaphoreType.DMA((2, 4, 2, 2, 2)),
            ],
            compiler_params=pltpu.CompilerParams(collective_id=0, has_side_effects=True, vmem_limit_bytes=62 * 2**20),
            name='two_site',
        )(x, left, mpo, right)

    return jax.shard_map(local_apply, mesh=mesh, in_specs=(P('bx', None, None, 'by'), P('bx', None, None), P(), P('by', None, None)), out_specs=P('bx', None, None, 'by'), check_vma=False)
```

```python
import functools

import jax
import jax.numpy as jnp
from jax import lax
from jax.experimental import pallas as pl
from jax.experimental.pallas import tpu as pltpu
from jax.sharding import PartitionSpec as P

HI = lax.Precision.HIGHEST
F32 = jnp.float32
LANE = 128
HALF = 64
GROUPS = 8
OWN, OTHER = 0, 1


def dot(a, b):
    return jnp.dot(a, b, precision=HI, preferred_element_type=F32)


def kernel(x_ref, l_ref, w_hbm, r_ref, y_ref, xg, ln, l2, rt, t1r, t1g, t3s, ys, yo, kron, w_ref, wa, wb, scale, load_sem, env_sem, out_sem, send_sem, recv_sem):
    by = lax.axis_index('by')
    bx = lax.axis_index('bx')
    core = lax.rem(bx, 2)
    chip = bx // 2
    sib = {'by': by, 'bx': bx + 1 - 2 * core}
    xnb = {'by': by, 'bx': lax.rem(bx + 2, 4)}
    ynb = {'by': 1 - by, 'bx': bx}

    def load(h, pq):
        i = h * 16 + pq
        return pltpu.make_async_copy(
            x_ref.at[:, pq // 4, pq % 4, pl.ds(h * LANE, LANE)],
            t1r.at[4, pl.ds(i // 8 * LANE, LANE), pl.ds(i % 8 * LANE, LANE)], load_sem.at[h, pq])

    for h in range(2):
        for pq in range(16):
            load(h, pq).start()
    env = []
    for half in range(2):
        for k in range(2):
            c0 = ((chip + half) % 2 * 2 + k) * LANE
            env.append(pltpu.make_async_copy(
                l_ref.at[:, :, pl.ds(pl.multiple_of(c0, LANE), LANE)], ln.at[half, k], env_sem.at[half * 2 + k]))
    for half in range(2):
        for h in range(2):
            f0 = ((by + half) % 2 * 2 + h) * LANE
            for r in range(4):
                env.append(pltpu.make_async_copy(
                    r_ref.at[:, r, pl.ds(pl.multiple_of(f0, LANE), LANE)],
                    t1r.at[3, pl.ds(half * 256, 256), pl.ds((h * 4 + r) * LANE, LANE)],
                    env_sem.at[4 + (half * 2 + h) * 4 + r]))
    env.append(pltpu.make_async_copy(w_hbm, w_ref, env_sem.at[20]))
    for cp in env:
        cp.start()

    barrier = pltpu.get_barrier_semaphore()
    for d in (sib, xnb, ynb):
        pl.semaphore_signal(barrier, inc=1, device_id=d, device_id_type=pl.DeviceIdType.MESH)
    pl.semaphore_wait(barrier, 3)

    def send(kind, g):
        fh, ch = ((0, 0), (0, 0), (0, 0), (0, 1), (1, 0), (1, 1), (1, 1), (0, 1), (1, 0))[kind]
        dh, dc = ((0, 1), (1, 0), (0, 0), (0, 1), (1, 0), (1, 1), (1, 1), (1, 1), (1, 1))[kind]
        to = (xnb, ynb, sib, sib, sib, sib, sib, ynb, xnb)[kind]
        part = pl.ds(*((0, 8), (0, 8), (0, 8), (0, 8), (0, 8), (0, 4), (4, 4), (0, 4), (4, 4))[kind])
        return pltpu.make_async_remote_copy(
            src_ref=xg.at[fh, g, ch, core, part],
            dst_ref=xg.at[dh, g, dc, core, part],
            send_sem=send_sem.at[kind, g],
            recv_sem=recv_sem.at[dh, g, dc, core, int(kind in (6, 8))],
            device_id=to, device_id_type=pl.DeviceIdType.MESH)

    def arrived(fh, ch, k, g, half=None):
        part = pl.ds(0, 8) if half is None else pl.ds(4 * half, 4)
        ref = xg.at[fh, g, ch, k, part]
        pltpu.make_async_copy(ref, ref, recv_sem.at[fh, g, ch, k, 0 if half is None else half]).wait()

    low = lax.broadcasted_iota(jnp.int32, (LANE, LANE), 1) < HALF

    def swap(v0, v1):
        m = low[:v0.shape[0]]
        return jnp.where(m, v0, pltpu.roll(v1, HALF, 1)), jnp.where(m, pltpu.roll(v0, HALF, 1), v1)

    def split(h):
        for pq in range(16):
            load(h, pq).wait()
        for n in range(8):
            blocks = [(h * 16 + pq) for pq in (2 * n, 2 * n + 1)]
            v = [t1r[4, i // 8 * LANE:(i // 8 + 1) * LANE, i % 8 * LANE:(i % 8 + 1) * LANE] for i in blocks]
            xg[OWN, 2 * h, OWN, core, n], xg[OWN, 2 * h + 1, OWN, core, n] = swap(*v)

    split(0)
    for g in range(2):
        for kind in range(3):
            send(kind, g).start()
    split(1)
    for g in range(2, 4):
        send(2, g).start()

    def relay(g):
        arrived(OWN, OTHER, core, g)
        send(3, g).start()
        send(7, g).start()
        arrived(OTHER, OWN, core, g)
        send(4, g).start()
        send(8, g).start()

        @pl.when(g < 2)
        def _():
            send(0, g + 2).start()
            send(1, g + 2).start()

    def relay_diag(g):
        for half in range(2):
            arrived(OTHER, OTHER, core, g, half)
            send(5 + half, g).start()

    for cp in env[:4] + env[20:]:
        cp.wait()
    for half in range(2):
        for k in range(2):
            l2[half, :, k * LANE:(k + 1) * LANE] = ln[half, k].reshape(512, LANE)
    wa[...] = jnp.zeros_like(wa)
    wb[...] = jnp.zeros_like(wb)
    lane8 = lax.broadcasted_iota(jnp.int32, (8, LANE), 1)
    row8 = lax.broadcasted_iota(jnp.int32, (8, LANE), 0)
    lane16 = lax.broadcasted_iota(jnp.int32, (16, LANE), 1)
    row16 = lax.broadcasted_iota(jnp.int32, (16, LANE), 0)

    def fill(i, carry):
        va, vb = carry
        i0, i1, i2 = i // 16, i // 4 % 4, i % 4
        for i3 in range(4):
            val = w_ref[i0, i1, i2, i3]
            va = jnp.where((row8 == i1) & (lane8 == i0 * 16 + i2 * 4 + i3), val, va)
            vb = jnp.where((row16 == i3 * 4 + i1) & (lane16 == i0 * 4 + i2), val, vb)
        return va, vb

    va, vb = lax.fori_loop(0, 64, fill, (jnp.zeros((8, LANE), F32), jnp.zeros((16, LANE), F32)), unroll=4)
    top = jnp.max(jnp.max(jnp.abs(va), axis=1, keepdims=True), axis=0, keepdims=True)
    scale[...] = jnp.broadcast_to(top, scale.shape)
    wa[...] = va / scale[...]
    wb[...] = vb / jnp.broadcast_to(top, (16, LANE))

    row = lax.broadcasted_iota(jnp.int32, (256, LANE), 0)
    a_mat = jnp.zeros((256, LANE), F32)
    for s in range(4):
        a_mat = jnp.where(row // 4 % 4 == s, wa[s:s + 1, :], a_mat)
    c_mat = jnp.zeros((256, LANE), F32)
    for rt_ in range(16):
        c_mat = jnp.where((row // 64) * 4 + row % 4 == rt_, wb[rt_:rt_ + 1, :], c_mat)
    col = lax.broadcasted_iota(jnp.int32, (LANE, 256), 1)
    pick = lax.broadcasted_iota(jnp.int32, (LANE, 256), 0)
    total = jnp.zeros((256, 256), F32)
    for v in range(4):
        left = dot(a_mat, jnp.where(pick == col % 4 * 16 + col // 64 * 4 + v, 1.0, 0.0).astype(F32))
        right = dot(c_mat, jnp.where(pick == v * 4 + col // 16 % 4, 1.0, 0.0).astype(F32))
        total = total + left * right
    krow = lax.broadcasted_iota(jnp.int32, (256, 256), 0)
    kcol = lax.broadcasted_iota(jnp.int32, (256, 256), 1)
    kron[...] = jnp.where(krow // 16 % 4 == kcol // 4 % 4, total, 0.0)
    for cp in env[4:20]:
        cp.wait()
    for fc in range(4):
        for r in range(4):
            t = t1r[3, fc // 2 * 256:(fc // 2 + 1) * 256, (fc % 2 * 4 + r) * LANE:(fc % 2 * 4 + r + 1) * LANE].T
            rt[fc * 2, r * HALF:(r + 1) * HALF, :] = t[:HALF]
            rt[fc * 2 + 1, r * HALF:(r + 1) * HALF, :] = t[HALF:]

    def stage1(fh, ch, g, first):
        xs = jnp.concatenate([
            jnp.concatenate([xg[fh, g, ch, k, n] for n in range(8)], axis=1) for k in range(2)], axis=0)
        t = dot(l2[ch], xs)
        buf = g if fh == 0 else lax.rem(g + 4, 5)
        if first:
            t1r[buf] = t
            return
        for n in range(8):
            lanes = slice(n * LANE, (n + 1) * LANE)
            for m in range(2):
                v = [t[ab * LANE:(ab + 1) * LANE, lanes] + t1r[buf, ab * LANE:(ab + 1) * LANE, lanes] for ab in (2 * m, 2 * m + 1)]
                for qb, w in enumerate(swap(*v)):
                    t1g[:, (2 * n + qb) * 16:(2 * n + qb + 1) * 16, m * LANE:(m + 1) * LANE] = (w * scale[0:1, 0:1]).reshape(GROUPS, 16, LANE)

    def stage2(g):
        sc = scale[0:1, 0:1]

        def body(_, c):
            for i in range(GROUPS):
                t = dot(kron[...], t1g[i]) * sc
                for rp in range(2):
                    for m in range(2):
                        v = [t[r * HALF:(r + 1) * HALF, m * LANE:(m + 1) * LANE] for r in (2 * rp, 2 * rp + 1)]
                        for n, w in enumerate(swap(*v)):
                            row0 = (2 * m + n) * 512 + i * 64
                            t3s[row0:row0 + 64, rp * LANE:(rp + 1) * LANE] = w
            return c

        lax.fori_loop(g, g + 1, body, 0)

    def stage3(fh, g, final=False):
        def body(_, c):
            part = dot(t3s[...], rt[fh * 4 + g])
            for b in range(2):
                v = part[:, b * LANE:(b + 1) * LANE]
                v = v + (jnp.where(g == 0, 0.0, ys[b]) if fh == 0 else ys[b])
                if final:
                    yo[b] = v.reshape(128, 4, 4, LANE)
                else:
                    ys[b] = v
            return c

        lax.fori_loop(g, g + 1, body, 0)

    other_core = 1 - core

    def own(i, _):
        for j in range(2):
            arrived(OWN, OWN, other_core, 2 * i + j)
        for j in range(2):
            stage1(OWN, OWN, 2 * i + j, True)
        return 0

    lax.fori_loop(0, 2, own, 0)

    def diagonal(g):
        for half in range(2):
            arrived(OTHER, OTHER, other_core, g, half)
        stage1(OTHER, OTHER, g, False)
        stage2(g)

    def direct(g, _):
        relay(g)
        arrived(OWN, OTHER, other_core, g)
        arrived(OTHER, OWN, other_core, g)
        stage1(OWN, OTHER, g, False)
        stage1(OTHER, OWN, g, True)
        stage2(g)
        pl.when(g > 0)(lambda: relay_diag(g - 1))
        stage3(OWN, g)

        @pl.when(g > 0)
        def _():
            diagonal(g - 1)
            pl.when(g == 3)(lambda: relay_diag(g))
            stage3(OTHER, g - 1)

        return 0

    lax.fori_loop(0, 4, direct, 0)

    def rest(g, _):
        diagonal(g)
        stage3(OTHER, g, True)
        return 0

    lax.fori_loop(3, 4, rest, 0)

    outs = [pltpu.make_async_copy(yo.at[b], y_ref.at[:, :, :, pl.ds(b * LANE, LANE)], out_sem.at[b]) for b in range(2)]
    for cp in outs:
        cp.start()
    for cp in outs:
        cp.wait()
    for kind in range(9):
        for g in range(4):
            send(kind, g).wait_send()


def solution(mesh):
    def local_apply(x, left, mpo, right):
        any_spec = pl.BlockSpec(memory_space=pl.ANY)
        return pl.pallas_call(
            kernel,
            out_shape=jax.ShapeDtypeStruct((128, 4, 4, 256), F32),
            in_specs=[any_spec] * 4,
            out_specs=any_spec,
            scratch_shapes=[
                pltpu.VMEM((2, 4, 2, 2, 8, 128, LANE), F32),
                pltpu.VMEM((2, 2, 128, 4, LANE), F32),
                pltpu.VMEM((2, 512, 256), F32),
                pltpu.VMEM((8, 256, 256), F32),
                pltpu.VMEM((5, 512, 1024), F32),
                pltpu.VMEM((GROUPS, 256, 256), F32),
                pltpu.VMEM((2048, 256), F32),
                pltpu.VMEM((2, 2048, LANE), F32),
                pltpu.VMEM((2, 128, 4, 4, LANE), F32),
                pltpu.VMEM((256, 256), F32),
                pltpu.SMEM((4, 4, 4, 4), F32),
                pltpu.VMEM((8, LANE), F32),
                pltpu.VMEM((16, LANE), F32),
                pltpu.VMEM((8, LANE), F32),
                pltpu.SemaphoreType.DMA((2, 16)),
                pltpu.SemaphoreType.DMA((21,)),
                pltpu.SemaphoreType.DMA((2,)),
                pltpu.SemaphoreType.DMA((9, 4)),
                pltpu.SemaphoreType.DMA((2, 4, 2, 2, 2)),
            ],
            compiler_params=pltpu.CompilerParams(collective_id=0, has_side_effects=True, vmem_limit_bytes=62 * 2**20),
            name='two_site',
        )(x, left, mpo, right)

    return jax.shard_map(local_apply, mesh=mesh, in_specs=(P('bx', None, None, 'by'), P('bx', None, None), P(), P('by', None, None)), out_specs=P('bx', None, None, 'by'), check_vma=False)
```

```python
import functools

import jax
import jax.numpy as jnp
from jax import lax
from jax.experimental import pallas as pl
from jax.experimental.pallas import tpu as pltpu
from jax.sharding import PartitionSpec as P

HI = lax.Precision.HIGHEST
F32 = jnp.float32
LANE = 128
HALF = 64
GROUPS = 8
OWN, OTHER = 0, 1


def dot(a, b):
    return jnp.dot(a, b, precision=HI, preferred_element_type=F32)


def kernel(x_ref, l_ref, w_hbm, r_ref, y_ref, xg, ln, l2, rt, t1r, t1g, t3s, ys, yo, kron, w_ref, wa, wb, scale, load_sem, env_sem, out_sem, send_sem, recv_sem):
    by = lax.axis_index('by')
    bx = lax.axis_index('bx')
    core = lax.rem(bx, 2)
    chip = bx // 2
    sib = {'by': by, 'bx': bx + 1 - 2 * core}
    xnb = {'by': by, 'bx': lax.rem(bx + 2, 4)}
    ynb = {'by': 1 - by, 'bx': bx}

    def load(h, pq):
        i = h * 16 + pq
        return pltpu.make_async_copy(
            x_ref.at[:, pq // 4, pq % 4, pl.ds(h * LANE, LANE)],
            t1r.at[4, pl.ds(i // 8 * LANE, LANE), pl.ds(i % 8 * LANE, LANE)], load_sem.at[h, pq])

    for h in range(2):
        for pq in range(16):
            load(h, pq).start()
    barrier = pltpu.get_barrier_semaphore()
    for d in (sib, xnb, ynb):
        pl.semaphore_signal(barrier, inc=1, device_id=d, device_id_type=pl.DeviceIdType.MESH)
    def send(kind, g):
        fh, ch = ((0, 0), (0, 0), (0, 0), (0, 1), (1, 0), (1, 1), (1, 1), (0, 1), (1, 0))[kind]
        dh, dc = ((0, 1), (1, 0), (0, 0), (0, 1), (1, 0), (1, 1), (1, 1), (1, 1), (1, 1))[kind]
        to = (xnb, ynb, sib, sib, sib, sib, sib, ynb, xnb)[kind]
        part = pl.ds(*((0, 8), (0, 8), (0, 8), (0, 8), (0, 8), (0, 4), (4, 4), (0, 4), (4, 4))[kind])
        return pltpu.make_async_remote_copy(
            src_ref=xg.at[fh, g, ch, core, part],
            dst_ref=xg.at[dh, g, dc, core, part],
            send_sem=send_sem.at[kind, g],
            recv_sem=recv_sem.at[dh, g, dc, core, int(kind in (6, 8))],
            device_id=to, device_id_type=pl.DeviceIdType.MESH)

    def arrived(fh, ch, k, g, half=None):
        part = pl.ds(0, 8) if half is None else pl.ds(4 * half, 4)
        ref = xg.at[fh, g, ch, k, part]
        pltpu.make_async_copy(ref, ref, recv_sem.at[fh, g, ch, k, 0 if half is None else half]).wait()

    low = lax.broadcasted_iota(jnp.int32, (LANE, LANE), 1) < HALF

    def swap(v0, v1):
        m = low[:v0.shape[0]]
        return jnp.where(m, v0, pltpu.roll(v1, HALF, 1)), jnp.where(m, pltpu.roll(v0, HALF, 1), v1)

    def split(h):
        for pq in range(16):
            load(h, pq).wait()
        for n in range(8):
            blocks = [(h * 16 + pq) for pq in (2 * n, 2 * n + 1)]
            v = [t1r[4, i // 8 * LANE:(i // 8 + 1) * LANE, i % 8 * LANE:(i % 8 + 1) * LANE] for i in blocks]
            xg[OWN, 2 * h, OWN, core, n], xg[OWN, 2 * h + 1, OWN, core, n] = swap(*v)

    split(0)
    pl.semaphore_wait(barrier, 3)
    for g in range(2):
        for kind in range(3):
            send(kind, g).start()
    env = []
    for half in range(2):
        for k in range(2):
            c0 = ((chip + half) % 2 * 2 + k) * LANE
            env.append(pltpu.make_async_copy(
                l_ref.at[:, :, pl.ds(pl.multiple_of(c0, LANE), LANE)], ln.at[half, k], env_sem.at[half * 2 + k]))
    for half in range(2):
        for h in range(2):
            f0 = ((by + half) % 2 * 2 + h) * LANE
            for r in range(4):
                env.append(pltpu.make_async_copy(
                    r_ref.at[:, r, pl.ds(pl.multiple_of(f0, LANE), LANE)],
                    t1r.at[3, pl.ds(half * 256, 256), pl.ds((h * 4 + r) * LANE, LANE)],
                    env_sem.at[4 + (half * 2 + h) * 4 + r]))
    env.append(pltpu.make_async_copy(w_hbm, w_ref, env_sem.at[20]))
    for cp in env:
        cp.start()


    split(1)
    for g in range(2, 4):
        send(2, g).start()

    def relay(g):
        arrived(OWN, OTHER, core, g)
        send(3, g).start()
        send(7, g).start()
        arrived(OTHER, OWN, core, g)
        send(4, g).start()
        send(8, g).start()

        @pl.when(g < 2)
        def _():
            send(0, g + 2).start()
            send(1, g + 2).start()

    def relay_diag(g):
        for half in range(2):
            arrived(OTHER, OTHER, core, g, half)
            send(5 + half, g).start()

    for cp in env[:4] + env[20:]:
        cp.wait()
    for half in range(2):
        for k in range(2):
            l2[half, :, k * LANE:(k + 1) * LANE] = ln[half, k].reshape(512, LANE)
    wa[...] = jnp.zeros_like(wa)
    wb[...] = jnp.zeros_like(wb)
    lane8 = lax.broadcasted_iota(jnp.int32, (8, LANE), 1)
    row8 = lax.broadcasted_iota(jnp.int32, (8, LANE), 0)
    lane16 = lax.broadcasted_iota(jnp.int32, (16, LANE), 1)
    row16 = lax.broadcasted_iota(jnp.int32, (16, LANE), 0)

    def fill(i, carry):
        va, vb = carry
        i0, i1, i2 = i // 16, i // 4 % 4, i % 4
        for i3 in range(4):
            val = w_ref[i0, i1, i2, i3]
            va = jnp.where((row8 == i1) & (lane8 == i0 * 16 + i2 * 4 + i3), val, va)
            vb = jnp.where((row16 == i3 * 4 + i1) & (lane16 == i0 * 4 + i2), val, vb)
        return va, vb

    va, vb = lax.fori_loop(0, 64, fill, (jnp.zeros((8, LANE), F32), jnp.zeros((16, LANE), F32)), unroll=4)
    top = jnp.max(jnp.max(jnp.abs(va), axis=1, keepdims=True), axis=0, keepdims=True)
    scale[...] = jnp.broadcast_to(top, scale.shape)
    wa[...] = va / scale[...]
    wb[...] = vb / jnp.broadcast_to(top, (16, LANE))

    row = lax.broadcasted_iota(jnp.int32, (256, LANE), 0)
    a_mat = jnp.zeros((256, LANE), F32)
    for s in range(4):
        a_mat = jnp.where(row // 4 % 4 == s, wa[s:s + 1, :], a_mat)
    c_mat = jnp.zeros((256, LANE), F32)
    for rt_ in range(16):
        c_mat = jnp.where((row // 64) * 4 + row % 4 == rt_, wb[rt_:rt_ + 1, :], c_mat)
    col = lax.broadcasted_iota(jnp.int32, (LANE, 256), 1)
    pick = lax.broadcasted_iota(jnp.int32, (LANE, 256), 0)
    total = jnp.zeros((256, 256), F32)
    for v in range(4):
        left = dot(a_mat, jnp.where(pick == col % 4 * 16 + col // 64 * 4 + v, 1.0, 0.0).astype(F32))
        right = dot(c_mat, jnp.where(pick == v * 4 + col // 16 % 4, 1.0, 0.0).astype(F32))
        total = total + left * right
    krow = lax.broadcasted_iota(jnp.int32, (256, 256), 0)
    kcol = lax.broadcasted_iota(jnp.int32, (256, 256), 1)
    kron[...] = jnp.where(krow // 16 % 4 == kcol // 4 % 4, total, 0.0)
    for cp in env[4:20]:
        cp.wait()
    for fc in range(4):
        for r in range(4):
            t = t1r[3, fc // 2 * 256:(fc // 2 + 1) * 256, (fc % 2 * 4 + r) * LANE:(fc % 2 * 4 + r + 1) * LANE].T
            rt[fc * 2, r * HALF:(r + 1) * HALF, :] = t[:HALF]
            rt[fc * 2 + 1, r * HALF:(r + 1) * HALF, :] = t[HALF:]

    def stage1(fh, ch, g, first):
        xs = jnp.concatenate([
            jnp.concatenate([xg[fh, g, ch, k, n] for n in range(8)], axis=1) for k in range(2)], axis=0)
        t = dot(l2[ch], xs)
        buf = g if fh == 0 else lax.rem(g + 4, 5)
        if first:
            t1r[buf] = t
            return
        for n in range(8):
            lanes = slice(n * LANE, (n + 1) * LANE)
            for m in range(2):
                v = [t[ab * LANE:(ab + 1) * LANE, lanes] + t1r[buf, ab * LANE:(ab + 1) * LANE, lanes] for ab in (2 * m, 2 * m + 1)]
                for qb, w in enumerate(swap(*v)):
                    t1g[:, (2 * n + qb) * 16:(2 * n + qb + 1) * 16, m * LANE:(m + 1) * LANE] = (w * scale[0:1, 0:1]).reshape(GROUPS, 16, LANE)

    def stage2(g):
        sc = scale[0:1, 0:1]

        def body(_, c):
            for i in range(GROUPS):
                t = dot(kron[...], t1g[i]) * sc
                for rp in range(2):
                    for m in range(2):
                        v = [t[r * HALF:(r + 1) * HALF, m * LANE:(m + 1) * LANE] for r in (2 * rp, 2 * rp + 1)]
                        for n, w in enumerate(swap(*v)):
                            row0 = (2 * m + n) * 512 + i * 64
                            t3s[row0:row0 + 64, rp * LANE:(rp + 1) * LANE] = w
            return c

        lax.fori_loop(g, g + 1, body, 0)

    def stage3(fh, g, final=False):
        def body(i, c):
            rows = pl.ds(i * 1024, 1024) if final else pl.ds(0, 2048)
            part = dot(t3s[rows, :], rt[fh * 4 + g])
            for b in range(2):
                v = part[:, b * LANE:(b + 1) * LANE]
                v = v + (jnp.where(g == 0, 0.0, ys[b, rows]) if fh == 0 else ys[b, rows])
                if final:
                    yo[b, pl.ds(i * 64, 64)] = v.reshape(64, 4, 4, LANE)
                    out_copy(b, i).start()
                else:
                    ys[b] = v
            return c

        if final:
            lax.fori_loop(0, 2, body, 0)
        else:
            lax.fori_loop(g, g + 1, body, 0)

    def out_copy(b, i):
        part = pl.ds(i * 64, 64)
        return pltpu.make_async_copy(yo.at[b, part], y_ref.at[part, :, :, pl.ds(b * LANE, LANE)], out_sem.at[b, i])

    other_core = 1 - core

    def own(i, _):
        for j in range(2):
            arrived(OWN, OWN, other_core, 2 * i + j)
        for j in range(2):
            stage1(OWN, OWN, 2 * i + j, True)
        return 0

    lax.fori_loop(0, 2, own, 0)

    def diagonal(g):
        for half in range(2):
            arrived(OTHER, OTHER, other_core, g, half)
        stage1(OTHER, OTHER, g, False)
        stage2(g)

    def direct(g, _):
        relay(g)
        arrived(OWN, OTHER, other_core, g)
        arrived(OTHER, OWN, other_core, g)
        stage1(OWN, OTHER, g, False)
        stage1(OTHER, OWN, g, True)
        stage2(g)
        pl.when(g > 0)(lambda: relay_diag(g - 1))
        stage3(OWN, g)

        @pl.when(g > 0)
        def _():
            diagonal(g - 1)
            pl.when(g == 3)(lambda: relay_diag(g))
            stage3(OTHER, g - 1)

        return 0

    lax.fori_loop(0, 4, direct, 0)

    def rest(g, _):
        diagonal(g)
        stage3(OTHER, g, True)
        return 0

    lax.fori_loop(3, 4, rest, 0)

    for kind in range(9):
        for g in range(4):
            send(kind, g).wait_send()
    for i in range(2):
        for b in range(2):
            out_copy(b, i).wait()


def solution(mesh):
    def local_apply(x, left, mpo, right):
        any_spec = pl.BlockSpec(memory_space=pl.ANY)
        return pl.pallas_call(
            kernel,
            out_shape=jax.ShapeDtypeStruct((128, 4, 4, 256), F32),
            in_specs=[any_spec] * 4,
            out_specs=any_spec,
            scratch_shapes=[
                pltpu.VMEM((2, 4, 2, 2, 8, 128, LANE), F32),
                pltpu.VMEM((2, 2, 128, 4, LANE), F32),
                pltpu.VMEM((2, 512, 256), F32),
                pltpu.VMEM((8, 256, 256), F32),
                pltpu.VMEM((5, 512, 1024), F32),
                pltpu.VMEM((GROUPS, 256, 256), F32),
                pltpu.VMEM((2048, 256), F32),
                pltpu.VMEM((2, 2048, LANE), F32),
                pltpu.VMEM((2, 128, 4, 4, LANE), F32),
                pltpu.VMEM((256, 256), F32),
                pltpu.SMEM((4, 4, 4, 4), F32),
                pltpu.VMEM((8, LANE), F32),
                pltpu.VMEM((16, LANE), F32),
                pltpu.VMEM((8, LANE), F32),
                pltpu.SemaphoreType.DMA((2, 16)),
                pltpu.SemaphoreType.DMA((21,)),
                pltpu.SemaphoreType.DMA((2, 2)),
                pltpu.SemaphoreType.DMA((9, 4)),
                pltpu.SemaphoreType.DMA((2, 4, 2, 2, 2)),
            ],
            compiler_params=pltpu.CompilerParams(collective_id=0, has_side_effects=True, vmem_limit_bytes=62 * 2**20),
            name='two_site',
        )(x, left, mpo, right)

    return jax.shard_map(local_apply, mesh=mesh, in_specs=(P('bx', None, None, 'by'), P('bx', None, None), P(), P('by', None, None)), out_specs=P('bx', None, None, 'by'), check_vma=False)
```

```python
import functools

import jax
import jax.numpy as jnp
from jax import lax
from jax.experimental import pallas as pl
from jax.experimental.pallas import tpu as pltpu
from jax.sharding import PartitionSpec as P

HI = lax.Precision.HIGHEST
F32 = jnp.float32
LANE = 128
HALF = 64
GROUPS = 8
OWN, OTHER = 0, 1


def dot(a, b):
    return jnp.dot(a, b, precision=HI, preferred_element_type=F32)


def kernel(x_ref, l_ref, w_hbm, r_ref, y_ref, xg, ln, l2, rt, t1r, t1g, t3s, ys, yo, kron, w_ref, wa, wb, scale, load_sem, env_sem, out_sem, send_sem, recv_sem):
    by = lax.axis_index('by')
    bx = lax.axis_index('bx')
    core = lax.rem(bx, 2)
    chip = bx // 2
    sib = {'by': by, 'bx': bx + 1 - 2 * core}
    xnb = {'by': by, 'bx': lax.rem(bx + 2, 4)}
    ynb = {'by': 1 - by, 'bx': bx}

    def load(h, pq):
        i = h * 16 + pq
        return pltpu.make_async_copy(
            x_ref.at[:, pq // 4, pq % 4, pl.ds(h * LANE, LANE)],
            t1r.at[4, pl.ds(i // 8 * LANE, LANE), pl.ds(i % 8 * LANE, LANE)], load_sem.at[h, pq])

    for h in range(2):
        for pq in range(16):
            load(h, pq).start()
    barrier = pltpu.get_barrier_semaphore()
    for d in (sib, xnb, ynb):
        pl.semaphore_signal(barrier, inc=1, device_id=d, device_id_type=pl.DeviceIdType.MESH)
    def send(kind, g, half):
        fh, ch = ((0, 0), (0, 0), (0, 0), (0, 1), (1, 0), (1, 1), (half, 1 - half))[kind]
        dh, dc = ((0, 1), (1, 0), (0, 0), (0, 1), (1, 0), (1, 1), (1, 1))[kind]
        to = (xnb, ynb, sib, sib, sib, sib, (ynb, xnb)[half])[kind]
        return pltpu.make_async_remote_copy(
            src_ref=xg.at[fh, g, ch, core, pl.ds(4 * half, 4)],
            dst_ref=xg.at[dh, g, dc, core, pl.ds(4 * half, 4)],
            send_sem=send_sem.at[kind, g, half],
            recv_sem=recv_sem.at[dh, g, dc, core, half],
            device_id=to, device_id_type=pl.DeviceIdType.MESH)

    def arrived(fh, ch, k, g, half):
        ref = xg.at[fh, g, ch, k, pl.ds(4 * half, 4)]
        pltpu.make_async_copy(ref, ref, recv_sem.at[fh, g, ch, k, half]).wait()

    def all_arrived(fh, ch, g):
        for half in range(2):
            arrived(fh, ch, 1 - core, g, half)

    def direct_sends(g):
        for half in range(2):
            send(0, g, half).start()
            send(1, g, half).start()

    low = lax.broadcasted_iota(jnp.int32, (LANE, LANE), 1) < HALF

    def swap(v0, v1):
        m = low[:v0.shape[0]]
        return jnp.where(m, v0, pltpu.roll(v1, HALF, 1)), jnp.where(m, pltpu.roll(v0, HALF, 1), v1)

    def split(h):
        for pq in range(16):
            load(h, pq).wait()
        for n in range(8):
            blocks = [(h * 16 + pq) for pq in (2 * n, 2 * n + 1)]
            v = [t1r[4, i // 8 * LANE:(i // 8 + 1) * LANE, i % 8 * LANE:(i % 8 + 1) * LANE] for i in blocks]
            xg[OWN, 2 * h, OWN, core, n], xg[OWN, 2 * h + 1, OWN, core, n] = swap(*v)

    split(0)
    pl.semaphore_wait(barrier, 3)
    for g in range(2):
        direct_sends(g)
    for g in range(2):
        for half in range(2):
            send(2, g, half).start()
    env = []
    for half in range(2):
        for k in range(2):
            c0 = ((chip + half) % 2 * 2 + k) * LANE
            env.append(pltpu.make_async_copy(
                l_ref.at[:, :, pl.ds(pl.multiple_of(c0, LANE), LANE)], ln.at[half, k], env_sem.at[half * 2 + k]))
    for half in range(2):
        for h in range(2):
            f0 = ((by + half) % 2 * 2 + h) * LANE
            for r in range(4):
                env.append(pltpu.make_async_copy(
                    r_ref.at[:, r, pl.ds(pl.multiple_of(f0, LANE), LANE)],
                    t1r.at[3, pl.ds(half * 256, 256), pl.ds((h * 4 + r) * LANE, LANE)],
                    env_sem.at[4 + (half * 2 + h) * 4 + r]))
    env.append(pltpu.make_async_copy(w_hbm, w_ref, env_sem.at[20]))
    for cp in env:
        cp.start()


    split(1)
    for g in range(2, 4):
        for half in range(2):
            send(2, g, half).start()

    def relay(g):
        for half in range(2):
            arrived(OWN, OTHER, core, g, half)
            send(3, g, half).start()
            if half == 0:
                send(6, g, half).start()
            arrived(OTHER, OWN, core, g, half)
            send(4, g, half).start()
            if half == 1:
                send(6, g, half).start()
        pl.when(g < 2)(lambda: direct_sends(g + 2))

    def relay_diag(g):
        for half in range(2):
            arrived(OTHER, OTHER, core, g, half)
            send(5, g, half).start()

    for cp in env[:4] + env[20:]:
        cp.wait()
    for half in range(2):
        for k in range(2):
            l2[half, :, k * LANE:(k + 1) * LANE] = ln[half, k].reshape(512, LANE)
    wa[...] = jnp.zeros_like(wa)
    wb[...] = jnp.zeros_like(wb)
    lane8 = lax.broadcasted_iota(jnp.int32, (8, LANE), 1)
    row8 = lax.broadcasted_iota(jnp.int32, (8, LANE), 0)
    lane16 = lax.broadcasted_iota(jnp.int32, (16, LANE), 1)
    row16 = lax.broadcasted_iota(jnp.int32, (16, LANE), 0)

    def fill(i, carry):
        va, vb = carry
        i0, i1, i2 = i // 16, i // 4 % 4, i % 4
        for i3 in range(4):
            val = w_ref[i0, i1, i2, i3]
            va = jnp.where((row8 == i1) & (lane8 == i0 * 16 + i2 * 4 + i3), val, va)
            vb = jnp.where((row16 == i3 * 4 + i1) & (lane16 == i0 * 4 + i2), val, vb)
        return va, vb

    va, vb = lax.fori_loop(0, 64, fill, (jnp.zeros((8, LANE), F32), jnp.zeros((16, LANE), F32)), unroll=4)
    top = jnp.max(jnp.max(jnp.abs(va), axis=1, keepdims=True), axis=0, keepdims=True)
    scale[...] = jnp.broadcast_to(top, scale.shape)
    wa[...] = va / scale[...]
    wb[...] = vb / jnp.broadcast_to(top, (16, LANE))

    row = lax.broadcasted_iota(jnp.int32, (256, LANE), 0)
    a_mat = jnp.zeros((256, LANE), F32)
    for s in range(4):
        a_mat = jnp.where(row // 4 % 4 == s, wa[s:s + 1, :], a_mat)
    c_mat = jnp.zeros((256, LANE), F32)
    for rt_ in range(16):
        c_mat = jnp.where((row // 64) * 4 + row % 4 == rt_, wb[rt_:rt_ + 1, :], c_mat)
    col = lax.broadcasted_iota(jnp.int32, (LANE, 256), 1)
    pick = lax.broadcasted_iota(jnp.int32, (LANE, 256), 0)
    total = jnp.zeros((256, 256), F32)
    for v in range(4):
        left = dot(a_mat, jnp.where(pick == col % 4 * 16 + col // 64 * 4 + v, 1.0, 0.0).astype(F32))
        right = dot(c_mat, jnp.where(pick == v * 4 + col // 16 % 4, 1.0, 0.0).astype(F32))
        total = total + left * right
    krow = lax.broadcasted_iota(jnp.int32, (256, 256), 0)
    kcol = lax.broadcasted_iota(jnp.int32, (256, 256), 1)
    kron[...] = jnp.where(krow // 16 % 4 == kcol // 4 % 4, total, 0.0)
    for cp in env[4:20]:
        cp.wait()
    for fc in range(4):
        for r in range(4):
            t = t1r[3, fc // 2 * 256:(fc // 2 + 1) * 256, (fc % 2 * 4 + r) * LANE:(fc % 2 * 4 + r + 1) * LANE].T
            rt[fc * 2, r * HALF:(r + 1) * HALF, :] = t[:HALF]
            rt[fc * 2 + 1, r * HALF:(r + 1) * HALF, :] = t[HALF:]

    def stage1(fh, ch, g, first):
        xs = jnp.concatenate([
            jnp.concatenate([xg[fh, g, ch, k, n] for n in range(8)], axis=1) for k in range(2)], axis=0)
        t = dot(l2[ch], xs)
        buf = g if fh == 0 else lax.rem(g + 4, 5)
        if first:
            t1r[buf] = t
            return
        for n in range(8):
            lanes = slice(n * LANE, (n + 1) * LANE)
            for m in range(2):
                v = [t[ab * LANE:(ab + 1) * LANE, lanes] + t1r[buf, ab * LANE:(ab + 1) * LANE, lanes] for ab in (2 * m, 2 * m + 1)]
                for qb, w in enumerate(swap(*v)):
                    t1g[:, (2 * n + qb) * 16:(2 * n + qb + 1) * 16, m * LANE:(m + 1) * LANE] = (w * scale[0:1, 0:1]).reshape(GROUPS, 16, LANE)

    def stage2(g):
        sc = scale[0:1, 0:1]

        def body(_, c):
            for i in range(GROUPS):
                t = dot(kron[...], t1g[i]) * sc
                for rp in range(2):
                    for m in range(2):
                        v = [t[r * HALF:(r + 1) * HALF, m * LANE:(m + 1) * LANE] for r in (2 * rp, 2 * rp + 1)]
                        for n, w in enumerate(swap(*v)):
                            row0 = (2 * m + n) * 512 + i * 64
                            t3s[row0:row0 + 64, rp * LANE:(rp + 1) * LANE] = w
            return c

        lax.fori_loop(g, g + 1, body, 0)

    def stage3(fh, g, final=False):
        def body(i, c):
            rows = pl.ds(i * 1024, 1024) if final else pl.ds(0, 2048)
            part = dot(t3s[rows, :], rt[fh * 4 + g])
            for b in range(2):
                v = part[:, b * LANE:(b + 1) * LANE]
                v = v + (jnp.where(g == 0, 0.0, ys[b, rows]) if fh == 0 else ys[b, rows])
                if final:
                    yo[b, pl.ds(i * 64, 64)] = v.reshape(64, 4, 4, LANE)
                    out_copy(b, i).start()
                else:
                    ys[b] = v
            return c

        if final:
            lax.fori_loop(0, 2, body, 0)
        else:
            lax.fori_loop(g, g + 1, body, 0)

    def out_copy(b, i):
        part = pl.ds(i * 64, 64)
        return pltpu.make_async_copy(yo.at[b, part], y_ref.at[part, :, :, pl.ds(b * LANE, LANE)], out_sem.at[b, i])

    def own(i, _):
        for j in range(2):
            all_arrived(OWN, OWN, 2 * i + j)
        for j in range(2):
            stage1(OWN, OWN, 2 * i + j, True)
        return 0

    lax.fori_loop(0, 2, own, 0)

    def diagonal(g):
        all_arrived(OTHER, OTHER, g)
        stage1(OTHER, OTHER, g, False)
        stage2(g)

    def direct(g, _):
        relay(g)
        all_arrived(OWN, OTHER, g)
        all_arrived(OTHER, OWN, g)
        stage1(OWN, OTHER, g, False)
        stage1(OTHER, OWN, g, True)
        stage2(g)
        pl.when(g > 0)(lambda: relay_diag(g - 1))
        stage3(OWN, g)

        @pl.when(g > 0)
        def _():
            diagonal(g - 1)
            pl.when(g == 3)(lambda: relay_diag(g))
            stage3(OTHER, g - 1)

        return 0

    lax.fori_loop(0, 4, direct, 0)

    def rest(g, _):
        diagonal(g)
        stage3(OTHER, g, True)
        return 0

    lax.fori_loop(3, 4, rest, 0)

    for kind in range(7):
        for g in range(4):
            for half in range(2):
                send(kind, g, half).wait_send()
    for i in range(2):
        for b in range(2):
            out_copy(b, i).wait()


def solution(mesh):
    def local_apply(x, left, mpo, right):
        any_spec = pl.BlockSpec(memory_space=pl.ANY)
        return pl.pallas_call(
            kernel,
            out_shape=jax.ShapeDtypeStruct((128, 4, 4, 256), F32),
            in_specs=[any_spec] * 4,
            out_specs=any_spec,
            scratch_shapes=[
                pltpu.VMEM((2, 4, 2, 2, 8, 128, LANE), F32),
                pltpu.VMEM((2, 2, 128, 4, LANE), F32),
                pltpu.VMEM((2, 512, 256), F32),
                pltpu.VMEM((8, 256, 256), F32),
                pltpu.VMEM((5, 512, 1024), F32),
                pltpu.VMEM((GROUPS, 256, 256), F32),
                pltpu.VMEM((2048, 256), F32),
                pltpu.VMEM((2, 2048, LANE), F32),
                pltpu.VMEM((2, 128, 4, 4, LANE), F32),
                pltpu.VMEM((256, 256), F32),
                pltpu.SMEM((4, 4, 4, 4), F32),
                pltpu.VMEM((8, LANE), F32),
                pltpu.VMEM((16, LANE), F32),
                pltpu.VMEM((8, LANE), F32),
                pltpu.SemaphoreType.DMA((2, 16)),
                pltpu.SemaphoreType.DMA((21,)),
                pltpu.SemaphoreType.DMA((2, 2)),
                pltpu.SemaphoreType.DMA((7, 4, 2)),
                pltpu.SemaphoreType.DMA((2, 4, 2, 2, 2)),
            ],
            compiler_params=pltpu.CompilerParams(collective_id=0, has_side_effects=True, vmem_limit_bytes=62 * 2**20),
            name='two_site',
        )(x, left, mpo, right)

    return jax.shard_map(local_apply, mesh=mesh, in_specs=(P('bx', None, None, 'by'), P('bx', None, None), P(), P('by', None, None)), out_specs=P('bx', None, None, 'by'), check_vma=False)
```

```python
import functools

import jax
import jax.numpy as jnp
from jax import lax
from jax.experimental import pallas as pl
from jax.experimental.pallas import tpu as pltpu
from jax.sharding import PartitionSpec as P

HI = lax.Precision.HIGHEST
F32 = jnp.float32
LANE = 128
HALF = 64
GROUPS = 8
OWN, OTHER = 0, 1


def dot(a, b):
    return jnp.dot(a, b, precision=HI, preferred_element_type=F32)


def kernel(x_ref, l_ref, w_hbm, r_ref, y_ref, xg, ln, l2, rt, t1r, t1g, t3s, ys, yo, kron, w_ref, wa, wb, scale, load_sem, env_sem, out_sem, send_sem, recv_sem, dsend_sem, drecv_sem):
    by = lax.axis_index('by')
    bx = lax.axis_index('bx')
    core = lax.rem(bx, 2)
    chip = bx // 2
    sib = {'by': by, 'bx': bx + 1 - 2 * core}
    xnb = {'by': by, 'bx': lax.rem(bx + 2, 4)}
    ynb = {'by': 1 - by, 'bx': bx}

    def load(h, pq):
        i = h * 16 + pq
        return pltpu.make_async_copy(
            x_ref.at[:, pq // 4, pq % 4, pl.ds(h * LANE, LANE)],
            t1r.at[4, pl.ds(i // 8 * LANE, LANE), pl.ds(i % 8 * LANE, LANE)], load_sem.at[h, pq])

    for h in range(2):
        for pq in range(16):
            load(h, pq).start()
    barrier = pltpu.get_barrier_semaphore()
    for d in (sib, xnb, ynb):
        pl.semaphore_signal(barrier, inc=1, device_id=d, device_id_type=pl.DeviceIdType.MESH)
    def send(kind, g, half):
        fh, ch = ((0, 0), (0, 0), (0, 0), (0, 1), (1, 0))[kind]
        dh, dc = ((0, 1), (1, 0), (0, 0), (0, 1), (1, 0))[kind]
        return pltpu.make_async_remote_copy(
            src_ref=xg.at[fh, g, ch, core, pl.ds(4 * half, 4)],
            dst_ref=xg.at[dh, g, dc, core, pl.ds(4 * half, 4)],
            send_sem=send_sem.at[kind, g, half],
            recv_sem=recv_sem.at[dh, g, dc, core, half],
            device_id=(xnb, ynb, sib, sib, sib)[kind], device_id_type=pl.DeviceIdType.MESH)

    def send_diag(kind, g, half, sub):
        fh, ch = ((half, 1 - half), (1, 1))[kind]
        part = pl.ds(4 * half + 2 * sub, 2)
        over = {'by': lax.rem(by + 1 - half, 2), 'bx': lax.rem(bx + 2 * half, 4)}
        return pltpu.make_async_remote_copy(
            src_ref=xg.at[fh, g, ch, core, part],
            dst_ref=xg.at[1, g, 1, core, part],
            send_sem=dsend_sem.at[kind, g, half, sub],
            recv_sem=drecv_sem.at[g, core, half, sub],
            device_id=(over, sib)[kind], device_id_type=pl.DeviceIdType.MESH)

    def arrived(fh, ch, k, g, half):
        ref = xg.at[fh, g, ch, k, pl.ds(4 * half, 4)]
        pltpu.make_async_copy(ref, ref, recv_sem.at[fh, g, ch, k, half]).wait()

    def arrived_diag(k, g, sub):
        for half in range(2):
            ref = xg.at[1, g, 1, k, pl.ds(4 * half + 2 * sub, 2)]
            pltpu.make_async_copy(ref, ref, drecv_sem.at[g, k, half, sub]).wait()

    def all_arrived(fh, ch, g):
        for half in range(2):
            arrived(fh, ch, 1 - core, g, half)

    def direct_sends(g):
        for half in range(2):
            send(0, g, half).start()
            send(1, g, half).start()

    low = lax.broadcasted_iota(jnp.int32, (LANE, LANE), 1) < HALF

    def swap(v0, v1):
        m = low[:v0.shape[0]]
        return jnp.where(m, v0, pltpu.roll(v1, HALF, 1)), jnp.where(m, pltpu.roll(v0, HALF, 1), v1)

    def split(h):
        for pq in range(16):
            load(h, pq).wait()
        for n in range(8):
            blocks = [(h * 16 + pq) for pq in (2 * n, 2 * n + 1)]
            v = [t1r[4, i // 8 * LANE:(i // 8 + 1) * LANE, i % 8 * LANE:(i % 8 + 1) * LANE] for i in blocks]
            xg[OWN, 2 * h, OWN, core, n], xg[OWN, 2 * h + 1, OWN, core, n] = swap(*v)

    split(0)
    pl.semaphore_wait(barrier, 3)
    for g in range(2):
        direct_sends(g)
    for g in range(2):
        for half in range(2):
            send(2, g, half).start()
    env = []
    for half in range(2):
        for k in range(2):
            c0 = ((chip + half) % 2 * 2 + k) * LANE
            env.append(pltpu.make_async_copy(
                l_ref.at[:, :, pl.ds(pl.multiple_of(c0, LANE), LANE)], ln.at[half, k], env_sem.at[half * 2 + k]))
    for half in range(2):
        for h in range(2):
            f0 = ((by + half) % 2 * 2 + h) * LANE
            for r in range(4):
                env.append(pltpu.make_async_copy(
                    r_ref.at[:, r, pl.ds(pl.multiple_of(f0, LANE), LANE)],
                    t1r.at[3, pl.ds(half * 256, 256), pl.ds((h * 4 + r) * LANE, LANE)],
                    env_sem.at[4 + (half * 2 + h) * 4 + r]))
    env.append(pltpu.make_async_copy(w_hbm, w_ref, env_sem.at[20]))
    for cp in env:
        cp.start()


    split(1)
    for g in range(2, 4):
        for half in range(2):
            send(2, g, half).start()

    def relay(g, half):
        arrived(OWN, OTHER, core, g, half)
        send(3, g, half).start()
        arrived(OTHER, OWN, core, g, half)
        send(4, g, half).start()
        for sub in range(2):
            send_diag(0, g, half, sub).start()

    def relay_diag(g, sub):
        arrived_diag(core, g, sub)
        for half in range(2):
            send_diag(1, g, half, sub).start()

    for cp in env[:4] + env[20:]:
        cp.wait()
    for half in range(2):
        for k in range(2):
            l2[half, :, k * LANE:(k + 1) * LANE] = ln[half, k].reshape(512, LANE)
    wa[...] = jnp.zeros_like(wa)
    wb[...] = jnp.zeros_like(wb)
    lane8 = lax.broadcasted_iota(jnp.int32, (8, LANE), 1)
    row8 = lax.broadcasted_iota(jnp.int32, (8, LANE), 0)
    lane16 = lax.broadcasted_iota(jnp.int32, (16, LANE), 1)
    row16 = lax.broadcasted_iota(jnp.int32, (16, LANE), 0)

    def fill(i, carry):
        va, vb = carry
        i0, i1, i2 = i // 16, i // 4 % 4, i % 4
        for i3 in range(4):
            val = w_ref[i0, i1, i2, i3]
            va = jnp.where((row8 == i1) & (lane8 == i0 * 16 + i2 * 4 + i3), val, va)
            vb = jnp.where((row16 == i3 * 4 + i1) & (lane16 == i0 * 4 + i2), val, vb)
        return va, vb

    va, vb = lax.fori_loop(0, 64, fill, (jnp.zeros((8, LANE), F32), jnp.zeros((16, LANE), F32)), unroll=4)
    top = jnp.max(jnp.max(jnp.abs(va), axis=1, keepdims=True), axis=0, keepdims=True)
    scale[...] = jnp.broadcast_to(top, scale.shape)
    wa[...] = va / scale[...]
    wb[...] = vb / jnp.broadcast_to(top, (16, LANE))

    row = lax.broadcasted_iota(jnp.int32, (256, LANE), 0)
    a_mat = jnp.zeros((256, LANE), F32)
    for s in range(4):
        a_mat = jnp.where(row // 4 % 4 == s, wa[s:s + 1, :], a_mat)
    c_mat = jnp.zeros((256, LANE), F32)
    for rt_ in range(16):
        c_mat = jnp.where((row // 64) * 4 + row % 4 == rt_, wb[rt_:rt_ + 1, :], c_mat)
    col = lax.broadcasted_iota(jnp.int32, (LANE, 256), 1)
    pick = lax.broadcasted_iota(jnp.int32, (LANE, 256), 0)
    total = jnp.zeros((256, 256), F32)
    for v in range(4):
        left = dot(a_mat, jnp.where(pick == col % 4 * 16 + col // 64 * 4 + v, 1.0, 0.0).astype(F32))
        right = dot(c_mat, jnp.where(pick == v * 4 + col // 16 % 4, 1.0, 0.0).astype(F32))
        total = total + left * right
    krow = lax.broadcasted_iota(jnp.int32, (256, 256), 0)
    kcol = lax.broadcasted_iota(jnp.int32, (256, 256), 1)
    kron[...] = jnp.where(krow // 16 % 4 == kcol // 4 % 4, total, 0.0)
    for cp in env[4:20]:
        cp.wait()
    for fc in range(4):
        for r in range(4):
            t = t1r[3, fc // 2 * 256:(fc // 2 + 1) * 256, (fc % 2 * 4 + r) * LANE:(fc % 2 * 4 + r + 1) * LANE].T
            rt[fc * 2, r * HALF:(r + 1) * HALF, :] = t[:HALF]
            rt[fc * 2 + 1, r * HALF:(r + 1) * HALF, :] = t[HALF:]

    def stage1(fh, ch, g, first, pairs):
        xs = jnp.concatenate([
            jnp.concatenate([xg[fh, g, ch, k, n] for n in pairs], axis=1) for k in range(2)], axis=0)
        t = dot(l2[ch], xs)
        buf = g if fh == 0 else lax.rem(g + 4, 5)
        for i, n in enumerate(pairs):
            lanes = slice(i * LANE, (i + 1) * LANE)
            held = pl.ds(n * LANE if isinstance(n, int) else pl.multiple_of(n * LANE, LANE), LANE)
            if first:
                t1r[buf, :, held] = t[:, lanes]
                continue
            for m in range(2):
                v = [t[ab * LANE:(ab + 1) * LANE, lanes] + t1r[buf, ab * LANE:(ab + 1) * LANE, held] for ab in (2 * m, 2 * m + 1)]
                for qb, w in enumerate(swap(*v)):
                    row0 = (2 * n + qb) * 16
                    row0 = row0 if isinstance(n, int) else pl.multiple_of(row0, 16)
                    t1g[:, pl.ds(row0, 16), m * LANE:(m + 1) * LANE] = (w * scale[0:1, 0:1]).reshape(GROUPS, 16, LANE)

    def stage2(g):
        sc = scale[0:1, 0:1]

        def body(_, c):
            for i in range(GROUPS):
                t = dot(kron[...], t1g[i]) * sc
                for rp in range(2):
                    for m in range(2):
                        v = [t[r * HALF:(r + 1) * HALF, m * LANE:(m + 1) * LANE] for r in (2 * rp, 2 * rp + 1)]
                        for n, w in enumerate(swap(*v)):
                            row0 = (2 * m + n) * 512 + i * 64
                            t3s[row0:row0 + 64, rp * LANE:(rp + 1) * LANE] = w
            return c

        lax.fori_loop(g, g + 1, body, 0)

    def stage3(fh, g, final=False):
        def body(i, c):
            rows = pl.ds(i * 1024, 1024) if final else pl.ds(0, 2048)
            part = dot(t3s[rows, :], rt[fh * 4 + g])
            for b in range(2):
                v = part[:, b * LANE:(b + 1) * LANE]
                v = v + (jnp.where(g == 0, 0.0, ys[b, rows]) if fh == 0 else ys[b, rows])
                if final:
                    yo[b, pl.ds(i * 64, 64)] = v.reshape(64, 4, 4, LANE)
                    out_copy(b, i).start()
                else:
                    ys[b] = v
            return c

        if final:
            lax.fori_loop(0, 2, body, 0)
        else:
            lax.fori_loop(g, g + 1, body, 0)

    def out_copy(b, i):
        part = pl.ds(i * 64, 64)
        return pltpu.make_async_copy(yo.at[b, part], y_ref.at[part, :, :, pl.ds(b * LANE, LANE)], out_sem.at[b, i])

    def own(i, _):
        for j in range(2):
            all_arrived(OWN, OWN, 2 * i + j)
        for j in range(2):
            stage1(OWN, OWN, 2 * i + j, True, range(8))
        return 0

    lax.fori_loop(0, 2, own, 0)

    def direct_half(g, half):
        relay(g, half)
        arrived(OWN, OTHER, 1 - core, g, half)
        arrived(OTHER, OWN, 1 - core, g, half)
        pairs = [4 * half + n for n in range(4)]
        stage1(OWN, OTHER, g, False, pairs)
        stage1(OTHER, OWN, g, True, pairs)

    def direct(g, _):
        lax.fori_loop(0, 2, lambda half, c: (direct_half(g, half), c)[1], 0)
        pl.when(g < 2)(lambda: direct_sends(g + 2))
        stage2(g)

        @pl.when(g > 0)
        def _():
            for sub in range(2):
                relay_diag(g - 1, sub)

        stage3(OWN, g)

        @pl.when(g > 0)
        def _():
            for sub in range(2):
                arrived_diag(1 - core, g - 1, sub)
            stage1(OTHER, OTHER, g - 1, False, range(8))
            stage2(g - 1)
            pl.when(g == 3)(lambda: relay_diag(g, 0))
            stage3(OTHER, g - 1)

        return 0

    lax.fori_loop(0, 4, direct, 0)

    def rest(g, _):
        relay_diag(g, 1)
        for sub in range(2):
            arrived_diag(1 - core, g, sub)
            stage1(OTHER, OTHER, g, False, [2 * sub, 2 * sub + 1, 2 * sub + 4, 2 * sub + 5])
        stage2(g)
        stage3(OTHER, g, True)
        return 0

    lax.fori_loop(3, 4, rest, 0)

    for g in range(4):
        for half in range(2):
            for kind in range(5):
                send(kind, g, half).wait_send()
            for kind in range(2):
                for sub in range(2):
                    send_diag(kind, g, half, sub).wait_send()
    for i in range(2):
        for b in range(2):
            out_copy(b, i).wait()


def solution(mesh):
    def local_apply(x, left, mpo, right):
        any_spec = pl.BlockSpec(memory_space=pl.ANY)
        return pl.pallas_call(
            kernel,
            out_shape=jax.ShapeDtypeStruct((128, 4, 4, 256), F32),
            in_specs=[any_spec] * 4,
            out_specs=any_spec,
            scratch_shapes=[
                pltpu.VMEM((2, 4, 2, 2, 8, 128, LANE), F32),
                pltpu.VMEM((2, 2, 128, 4, LANE), F32),
                pltpu.VMEM((2, 512, 256), F32),
                pltpu.VMEM((8, 256, 256), F32),
                pltpu.VMEM((5, 512, 1024), F32),
                pltpu.VMEM((GROUPS, 256, 256), F32),
                pltpu.VMEM((2048, 256), F32),
                pltpu.VMEM((2, 2048, LANE), F32),
                pltpu.VMEM((2, 128, 4, 4, LANE), F32),
                pltpu.VMEM((256, 256), F32),
                pltpu.SMEM((4, 4, 4, 4), F32),
                pltpu.VMEM((8, LANE), F32),
                pltpu.VMEM((16, LANE), F32),
                pltpu.VMEM((8, LANE), F32),
                pltpu.SemaphoreType.DMA((2, 16)),
                pltpu.SemaphoreType.DMA((21,)),
                pltpu.SemaphoreType.DMA((2, 2)),
                pltpu.SemaphoreType.DMA((5, 4, 2)),
                pltpu.SemaphoreType.DMA((2, 4, 2, 2, 2)),
                pltpu.SemaphoreType.DMA((2, 4, 2, 2)),
                pltpu.SemaphoreType.DMA((4, 2, 2, 2)),
            ],
            compiler_params=pltpu.CompilerParams(collective_id=0, has_side_effects=True, vmem_limit_bytes=62 * 2**20),
            name='two_site',
        )(x, left, mpo, right)

    return jax.shard_map(local_apply, mesh=mesh, in_specs=(P('bx', None, None, 'by'), P('bx', None, None), P(), P('by', None, None)), out_specs=P('bx', None, None, 'by'), check_vma=False)
```

```python
import functools

import jax
import jax.numpy as jnp
from jax import lax
from jax.experimental import pallas as pl
from jax.experimental.pallas import tpu as pltpu
from jax.sharding import PartitionSpec as P

HI = lax.Precision.HIGHEST
F32 = jnp.float32
LANE = 128
HALF = 64
GROUPS = 8
OWN, OTHER = 0, 1


def dot(a, b):
    return jnp.dot(a, b, precision=HI, preferred_element_type=F32)


def kernel(x_ref, l_ref, w_hbm, r_ref, y_ref, xg, ln, l2, rt, t1r, t1g, t3s, ys, yo, kron, w_ref, wa, wb, scale, load_sem, env_sem, out_sem, send_sem, recv_sem):
    by = lax.axis_index('by')
    bx = lax.axis_index('bx')
    core = lax.rem(bx, 2)
    chip = bx // 2
    sib = {'by': by, 'bx': bx + 1 - 2 * core}
    xnb = {'by': by, 'bx': lax.rem(bx + 2, 4)}
    ynb = {'by': 1 - by, 'bx': bx}

    def load(h, pq):
        i = h * 16 + pq
        return pltpu.make_async_copy(
            x_ref.at[:, pq // 4, pq % 4, pl.ds(h * LANE, LANE)],
            t1r.at[4, pl.ds(i // 8 * LANE, LANE), pl.ds(i % 8 * LANE, LANE)], load_sem.at[h, pq])

    for h in range(2):
        for pq in range(16):
            load(h, pq).start()
    barrier = pltpu.get_barrier_semaphore()
    for d in (sib, xnb, ynb):
        pl.semaphore_signal(barrier, inc=1, device_id=d, device_id_type=pl.DeviceIdType.MESH)
    def pairs(half):
        return pl.ds(0, 8) if half is None else pl.ds(4 * half, 4)

    def send(kind, g, half=None):
        fh, ch = ((0, 0), (0, 0), (0, 0), (0, 1), (1, 0), (1, 1), (half, 1 - (half or 0)))[kind]
        dh, dc = ((0, 1), (1, 0), (0, 0), (0, 1), (1, 0), (1, 1), (1, 1))[kind]
        to = (xnb, ynb, sib, sib, sib, sib, (ynb, xnb)[half or 0])[kind]
        return pltpu.make_async_remote_copy(
            src_ref=xg.at[fh, g, ch, core, pairs(half)],
            dst_ref=xg.at[dh, g, dc, core, pairs(half)],
            send_sem=send_sem.at[kind, g, half or 0],
            recv_sem=recv_sem.at[dh, g, dc, core, half or 0],
            device_id=to, device_id_type=pl.DeviceIdType.MESH)

    def arrived(fh, ch, k, g, half=None):
        ref = xg.at[fh, g, ch, k, pairs(half)]
        pltpu.make_async_copy(ref, ref, recv_sem.at[fh, g, ch, k, half or 0]).wait()

    def parts(g):
        return (None,) if g < 3 else (0, 1)

    def direct_sends(g):
        for half in parts(g):
            send(0, g, half).start()
            send(1, g, half).start()

    low = lax.broadcasted_iota(jnp.int32, (LANE, LANE), 1) < HALF

    def swap(v0, v1):
        m = low[:v0.shape[0]]
        return jnp.where(m, v0, pltpu.roll(v1, HALF, 1)), jnp.where(m, pltpu.roll(v0, HALF, 1), v1)

    def split(h):
        for pq in range(16):
            load(h, pq).wait()
        for n in range(8):
            blocks = [(h * 16 + pq) for pq in (2 * n, 2 * n + 1)]
            v = [t1r[4, i // 8 * LANE:(i // 8 + 1) * LANE, i % 8 * LANE:(i % 8 + 1) * LANE] for i in blocks]
            xg[OWN, 2 * h, OWN, core, n], xg[OWN, 2 * h + 1, OWN, core, n] = swap(*v)

    split(0)
    pl.semaphore_wait(barrier, 3)
    for g in range(2):
        direct_sends(g)
    for g in range(2):
        send(2, g).start()
    env = []
    for half in range(2):
        for k in range(2):
            c0 = ((chip + half) % 2 * 2 + k) * LANE
            env.append(pltpu.make_async_copy(
                l_ref.at[:, :, pl.ds(pl.multiple_of(c0, LANE), LANE)], ln.at[half, k], env_sem.at[half * 2 + k]))
    for half in range(2):
        for h in range(2):
            f0 = ((by + half) % 2 * 2 + h) * LANE
            for r in range(4):
                env.append(pltpu.make_async_copy(
                    r_ref.at[:, r, pl.ds(pl.multiple_of(f0, LANE), LANE)],
                    t1r.at[3, pl.ds(half * 256, 256), pl.ds((h * 4 + r) * LANE, LANE)],
                    env_sem.at[4 + (half * 2 + h) * 4 + r]))
    env.append(pltpu.make_async_copy(w_hbm, w_ref, env_sem.at[20]))
    for cp in env:
        cp.start()


    split(1)
    for g in range(2, 4):
        send(2, g).start()

    def relay(g):
        @pl.when(g < 3)
        def _():
            arrived(OWN, OTHER, core, g)
            send(3, g).start()
            send(6, g, 0).start()
            arrived(OTHER, OWN, core, g)
            send(4, g).start()
            send(6, g, 1).start()
            pl.when(g == 0)(lambda: direct_sends(2))
            pl.when(g == 1)(lambda: direct_sends(3))
            arrived(OWN, OTHER, 1 - core, g)
            arrived(OTHER, OWN, 1 - core, g)

        @pl.when(g == 3)
        def _():
            for half in range(2):
                arrived(OWN, OTHER, core, g, half)
                send(3, g, half).start()
                if half == 0:
                    send(6, g, 0).start()
                arrived(OTHER, OWN, core, g, half)
                send(4, g, half).start()
                if half == 1:
                    send(6, g, 1).start()
            for half in range(2):
                arrived(OWN, OTHER, 1 - core, g, half)
                arrived(OTHER, OWN, 1 - core, g, half)

    def relay_diag(g):
        for half in range(2):
            arrived(OTHER, OTHER, core, g, half)
            send(5, g, half).start()

    for cp in env[:4] + env[20:]:
        cp.wait()
    for half in range(2):
        for k in range(2):
            l2[half, :, k * LANE:(k + 1) * LANE] = ln[half, k].reshape(512, LANE)
    wa[...] = jnp.zeros_like(wa)
    wb[...] = jnp.zeros_like(wb)
    lane8 = lax.broadcasted_iota(jnp.int32, (8, LANE), 1)
    row8 = lax.broadcasted_iota(jnp.int32, (8, LANE), 0)
    lane16 = lax.broadcasted_iota(jnp.int32, (16, LANE), 1)
    row16 = lax.broadcasted_iota(jnp.int32, (16, LANE), 0)

    def fill(i, carry):
        va, vb = carry
        i0, i1, i2 = i // 16, i // 4 % 4, i % 4
        for i3 in range(4):
            val = w_ref[i0, i1, i2, i3]
            va = jnp.where((row8 == i1) & (lane8 == i0 * 16 + i2 * 4 + i3), val, va)
            vb = jnp.where((row16 == i3 * 4 + i1) & (lane16 == i0 * 4 + i2), val, vb)
        return va, vb

    va, vb = lax.fori_loop(0, 64, fill, (jnp.zeros((8, LANE), F32), jnp.zeros((16, LANE), F32)), unroll=4)
    top = jnp.max(jnp.max(jnp.abs(va), axis=1, keepdims=True), axis=0, keepdims=True)
    scale[...] = jnp.broadcast_to(top, scale.shape)
    wa[...] = va / scale[...]
    wb[...] = vb / jnp.broadcast_to(top, (16, LANE))

    row = lax.broadcasted_iota(jnp.int32, (256, LANE), 0)
    a_mat = jnp.zeros((256, LANE), F32)
    for s in range(4):
        a_mat = jnp.where(row // 4 % 4 == s, wa[s:s + 1, :], a_mat)
    c_mat = jnp.zeros((256, LANE), F32)
    for rt_ in range(16):
        c_mat = jnp.where((row // 64) * 4 + row % 4 == rt_, wb[rt_:rt_ + 1, :], c_mat)
    col = lax.broadcasted_iota(jnp.int32, (LANE, 256), 1)
    pick = lax.broadcasted_iota(jnp.int32, (LANE, 256), 0)
    total = jnp.zeros((256, 256), F32)
    for v in range(4):
        left = dot(a_mat, jnp.where(pick == col % 4 * 16 + col // 64 * 4 + v, 1.0, 0.0).astype(F32))
        right = dot(c_mat, jnp.where(pick == v * 4 + col // 16 % 4, 1.0, 0.0).astype(F32))
        total = total + left * right
    krow = lax.broadcasted_iota(jnp.int32, (256, 256), 0)
    kcol = lax.broadcasted_iota(jnp.int32, (256, 256), 1)
    kron[...] = jnp.where(krow // 16 % 4 == kcol // 4 % 4, total, 0.0)
    for cp in env[4:20]:
        cp.wait()
    for fc in range(4):
        for r in range(4):
            t = t1r[3, fc // 2 * 256:(fc // 2 + 1) * 256, (fc % 2 * 4 + r) * LANE:(fc % 2 * 4 + r + 1) * LANE].T
            rt[fc * 2, r * HALF:(r + 1) * HALF, :] = t[:HALF]
            rt[fc * 2 + 1, r * HALF:(r + 1) * HALF, :] = t[HALF:]

    def stage1(fh, ch, g, first):
        xs = jnp.concatenate([
            jnp.concatenate([xg[fh, g, ch, k, n] for n in range(8)], axis=1) for k in range(2)], axis=0)
        t = dot(l2[ch], xs)
        buf = g if fh == 0 else lax.rem(g + 4, 5)
        if first:
            t1r[buf] = t
            return
        for n in range(8):
            lanes = slice(n * LANE, (n + 1) * LANE)
            for m in range(2):
                v = [t[ab * LANE:(ab + 1) * LANE, lanes] + t1r[buf, ab * LANE:(ab + 1) * LANE, lanes] for ab in (2 * m, 2 * m + 1)]
                for qb, w in enumerate(swap(*v)):
                    t1g[:, (2 * n + qb) * 16:(2 * n + qb + 1) * 16, m * LANE:(m + 1) * LANE] = (w * scale[0:1, 0:1]).reshape(GROUPS, 16, LANE)

    def stage2(g):
        sc = scale[0:1, 0:1]

        def body(_, c):
            for i in range(GROUPS):
                t = dot(kron[...], t1g[i]) * sc
                for rp in range(2):
                    for m in range(2):
                        v = [t[r * HALF:(r + 1) * HALF, m * LANE:(m + 1) * LANE] for r in (2 * rp, 2 * rp + 1)]
                        for n, w in enumerate(swap(*v)):
                            row0 = (2 * m + n) * 512 + i * 64
                            t3s[row0:row0 + 64, rp * LANE:(rp + 1) * LANE] = w
            return c

        lax.fori_loop(g, g + 1, body, 0)

    def stage3(fh, g, final=False):
        def body(i, c):
            rows = pl.ds(i * 1024, 1024) if final else pl.ds(0, 2048)
            part = dot(t3s[rows, :], rt[fh * 4 + g])
            for b in range(2):
                v = part[:, b * LANE:(b + 1) * LANE]
                v = v + (jnp.where(g == 0, 0.0, ys[b, rows]) if fh == 0 else ys[b, rows])
                if final:
                    yo[b, pl.ds(i * 64, 64)] = v.reshape(64, 4, 4, LANE)
                    out_copy(b, i).start()
                else:
                    ys[b] = v
            return c

        if final:
            lax.fori_loop(0, 2, body, 0)
        else:
            lax.fori_loop(g, g + 1, body, 0)

    def out_copy(b, i):
        part = pl.ds(i * 64, 64)
        return pltpu.make_async_copy(yo.at[b, part], y_ref.at[part, :, :, pl.ds(b * LANE, LANE)], out_sem.at[b, i])

    def own(i, _):
        for j in range(2):
            arrived(OWN, OWN, 1 - core, 2 * i + j)
        for j in range(2):
            stage1(OWN, OWN, 2 * i + j, True)
        return 0

    lax.fori_loop(0, 2, own, 0)

    def diagonal(g):
        for half in range(2):
            arrived(OTHER, OTHER, 1 - core, g, half)
        stage1(OTHER, OTHER, g, False)
        stage2(g)

    def direct(g, _):
        relay(g)
        stage1(OWN, OTHER, g, False)
        stage1(OTHER, OWN, g, True)
        stage2(g)
        pl.when(g > 0)(lambda: relay_diag(g - 1))
        stage3(OWN, g)

        @pl.when(g > 0)
        def _():
            diagonal(g - 1)
            pl.when(g == 3)(lambda: relay_diag(g))
            stage3(OTHER, g - 1)

        return 0

    lax.fori_loop(0, 4, direct, 0)

    def rest(g, _):
        diagonal(g)
        stage3(OTHER, g, True)
        return 0

    lax.fori_loop(3, 4, rest, 0)

    for g in range(4):
        for kind in range(7):
            for half in ((None,) if kind == 2 else (0, 1) if kind > 4 else parts(g)):
                send(kind, g, half).wait_send()
    for i in range(2):
        for b in range(2):
            out_copy(b, i).wait()


def solution(mesh):
    def local_apply(x, left, mpo, right):
        any_spec = pl.BlockSpec(memory_space=pl.ANY)
        return pl.pallas_call(
            kernel,
            out_shape=jax.ShapeDtypeStruct((128, 4, 4, 256), F32),
            in_specs=[any_spec] * 4,
            out_specs=any_spec,
            scratch_shapes=[
                pltpu.VMEM((2, 4, 2, 2, 8, 128, LANE), F32),
                pltpu.VMEM((2, 2, 128, 4, LANE), F32),
                pltpu.VMEM((2, 512, 256), F32),
                pltpu.VMEM((8, 256, 256), F32),
                pltpu.VMEM((5, 512, 1024), F32),
                pltpu.VMEM((GROUPS, 256, 256), F32),
                pltpu.VMEM((2048, 256), F32),
                pltpu.VMEM((2, 2048, LANE), F32),
                pltpu.VMEM((2, 128, 4, 4, LANE), F32),
                pltpu.VMEM((256, 256), F32),
                pltpu.SMEM((4, 4, 4, 4), F32),
                pltpu.VMEM((8, LANE), F32),
                pltpu.VMEM((16, LANE), F32),
                pltpu.VMEM((8, LANE), F32),
                pltpu.SemaphoreType.DMA((2, 16)),
                pltpu.SemaphoreType.DMA((21,)),
                pltpu.SemaphoreType.DMA((2, 2)),
                pltpu.SemaphoreType.DMA((7, 4, 2)),
                pltpu.SemaphoreType.DMA((2, 4, 2, 2, 2)),
            ],
            compiler_params=pltpu.CompilerParams(collective_id=0, has_side_effects=True, vmem_limit_bytes=62 * 2**20),
            name='two_site',
        )(x, left, mpo, right)

    return jax.shard_map(local_apply, mesh=mesh, in_specs=(P('bx', None, None, 'by'), P('bx', None, None), P(), P('by', None, None)), out_specs=P('bx', None, None, 'by'), check_vma=False)
```

```python
import functools

import jax
import jax.numpy as jnp
from jax import lax
from jax.experimental import pallas as pl
from jax.experimental.pallas import tpu as pltpu
from jax.sharding import PartitionSpec as P

HI = lax.Precision.HIGHEST
F32 = jnp.float32
LANE = 128
HALF = 64
GROUPS = 8
OWN, OTHER = 0, 1


def dot(a, b):
    return jnp.dot(a, b, precision=HI, preferred_element_type=F32)


def kernel(x_ref, l_ref, w_hbm, r_ref, y_ref, xg, ln, l2, rt, t1r, t1g, t3s, ys, yo, kron, w_ref, wa, wb, scale, load_sem, env_sem, out_sem, send_sem, recv_sem):
    by = lax.axis_index('by')
    bx = lax.axis_index('bx')
    core = lax.rem(bx, 2)
    chip = bx // 2
    sib = {'by': by, 'bx': bx + 1 - 2 * core}
    xnb = {'by': by, 'bx': lax.rem(bx + 2, 4)}
    ynb = {'by': 1 - by, 'bx': bx}

    def load(h, pq):
        i = h * 16 + pq
        return pltpu.make_async_copy(
            x_ref.at[:, pq // 4, pq % 4, pl.ds(h * LANE, LANE)],
            t1r.at[4, pl.ds(i // 8 * LANE, LANE), pl.ds(i % 8 * LANE, LANE)], load_sem.at[h, pq])

    for h in range(2):
        for pq in range(16):
            load(h, pq).start()
    barrier = pltpu.get_barrier_semaphore()
    for d in (sib, xnb, ynb):
        pl.semaphore_signal(barrier, inc=1, device_id=d, device_id_type=pl.DeviceIdType.MESH)
    def pairs(half):
        return pl.ds(0, 8) if half is None else pl.ds(4 * half, 4)

    def send(kind, g, half=None):
        h0 = 0 if half is None else half
        fh, ch = ((0, 0), (0, 0), (0, 0), (0, 1), (1, 0), (1, 1), (h0, 1 - h0))[kind]
        dh, dc = ((0, 1), (1, 0), (0, 0), (0, 1), (1, 0), (1, 1), (1, 1))[kind]
        to = (ynb, xnb)[half] if kind == 6 else (xnb, ynb, sib, sib, sib, sib)[kind]
        return pltpu.make_async_remote_copy(
            src_ref=xg.at[fh, g, ch, core, pairs(half)],
            dst_ref=xg.at[dh, g, dc, core, pairs(half)],
            send_sem=send_sem.at[kind, g, h0],
            recv_sem=recv_sem.at[dh, g, dc, core, h0],
            device_id=to, device_id_type=pl.DeviceIdType.MESH)

    def arrived(fh, ch, k, g, half=None):
        ref = xg.at[fh, g, ch, k, pairs(half)]
        pltpu.make_async_copy(ref, ref, recv_sem.at[fh, g, ch, k, 0 if half is None else half]).wait()

    def parts(g):
        return (None,) if g < 3 else (0, 1)

    def direct_sends(g):
        for half in parts(g):
            send(0, g, half).start()
            send(1, g, half).start()

    low = lax.broadcasted_iota(jnp.int32, (LANE, LANE), 1) < HALF

    def swap(v0, v1):
        m = low[:v0.shape[0]]
        return jnp.where(m, v0, pltpu.roll(v1, HALF, 1)), jnp.where(m, pltpu.roll(v0, HALF, 1), v1)

    def split(h):
        for pq in range(16):
            load(h, pq).wait()
        for n in range(8):
            blocks = [(h * 16 + pq) for pq in (2 * n, 2 * n + 1)]
            v = [t1r[4, i // 8 * LANE:(i // 8 + 1) * LANE, i % 8 * LANE:(i % 8 + 1) * LANE] for i in blocks]
            xg[OWN, 2 * h, OWN, core, n], xg[OWN, 2 * h + 1, OWN, core, n] = swap(*v)

    split(0)
    pl.semaphore_wait(barrier, 3)
    for g in range(2):
        direct_sends(g)
    for g in range(2):
        send(2, g).start()
    env = []
    for half in range(2):
        for k in range(2):
            c0 = ((chip + half) % 2 * 2 + k) * LANE
            env.append(pltpu.make_async_copy(
                l_ref.at[:, :, pl.ds(pl.multiple_of(c0, LANE), LANE)], ln.at[half, k], env_sem.at[half * 2 + k]))
    for half in range(2):
        for h in range(2):
            f0 = ((by + half) % 2 * 2 + h) * LANE
            for r in range(4):
                env.append(pltpu.make_async_copy(
                    r_ref.at[:, r, pl.ds(pl.multiple_of(f0, LANE), LANE)],
                    t1r.at[3, pl.ds(half * 256, 256), pl.ds((h * 4 + r) * LANE, LANE)],
                    env_sem.at[4 + (half * 2 + h) * 4 + r]))
    env.append(pltpu.make_async_copy(w_hbm, w_ref, env_sem.at[20]))
    for cp in env:
        cp.start()


    split(1)
    for g in range(2, 4):
        send(2, g).start()

    def relay(g):
        arrived(OWN, OTHER, core, g)
        send(3, g).start()
        send(6, g, 0).start()
        arrived(OTHER, OWN, core, g)
        send(4, g).start()
        send(6, g, 1).start()
        pl.when(g == 0)(lambda: direct_sends(2))
        pl.when(g == 1)(lambda: direct_sends(3))
        arrived(OWN, OTHER, 1 - core, g)
        arrived(OTHER, OWN, 1 - core, g)

    def relay_half(g, half):
        arrived(OWN, OTHER, core, g, half)
        send(3, g, half).start()
        pl.when(half == 0)(lambda: send(6, g, 0).start())
        arrived(OTHER, OWN, core, g, half)
        send(4, g, half).start()
        pl.when(half == 1)(lambda: send(6, g, 1).start())
        arrived(OWN, OTHER, 1 - core, g, half)
        arrived(OTHER, OWN, 1 - core, g, half)

    def relay_diag(g):
        for half in range(2):
            arrived(OTHER, OTHER, core, g, half)
            send(5, g, half).start()

    for cp in env[:4] + env[20:]:
        cp.wait()
    for half in range(2):
        for k in range(2):
            l2[half, :, k * LANE:(k + 1) * LANE] = ln[half, k].reshape(512, LANE)
    wa[...] = jnp.zeros_like(wa)
    wb[...] = jnp.zeros_like(wb)
    lane8 = lax.broadcasted_iota(jnp.int32, (8, LANE), 1)
    row8 = lax.broadcasted_iota(jnp.int32, (8, LANE), 0)
    lane16 = lax.broadcasted_iota(jnp.int32, (16, LANE), 1)
    row16 = lax.broadcasted_iota(jnp.int32, (16, LANE), 0)

    def fill(i, carry):
        va, vb = carry
        i0, i1, i2 = i // 16, i // 4 % 4, i % 4
        for i3 in range(4):
            val = w_ref[i0, i1, i2, i3]
            va = jnp.where((row8 == i1) & (lane8 == i0 * 16 + i2 * 4 + i3), val, va)
            vb = jnp.where((row16 == i3 * 4 + i1) & (lane16 == i0 * 4 + i2), val, vb)
        return va, vb

    va, vb = lax.fori_loop(0, 64, fill, (jnp.zeros((8, LANE), F32), jnp.zeros((16, LANE), F32)), unroll=4)
    top = jnp.max(jnp.max(jnp.abs(va), axis=1, keepdims=True), axis=0, keepdims=True)
    scale[...] = jnp.broadcast_to(top, scale.shape)
    wa[...] = va / scale[...]
    wb[...] = vb / jnp.broadcast_to(top, (16, LANE))

    row = lax.broadcasted_iota(jnp.int32, (256, LANE), 0)
    a_mat = jnp.zeros((256, LANE), F32)
    for s in range(4):
        a_mat = jnp.where(row // 4 % 4 == s, wa[s:s + 1, :], a_mat)
    c_mat = jnp.zeros((256, LANE), F32)
    for rt_ in range(16):
        c_mat = jnp.where((row // 64) * 4 + row % 4 == rt_, wb[rt_:rt_ + 1, :], c_mat)
    col = lax.broadcasted_iota(jnp.int32, (LANE, 256), 1)
    pick = lax.broadcasted_iota(jnp.int32, (LANE, 256), 0)
    total = jnp.zeros((256, 256), F32)
    for v in range(4):
        left = dot(a_mat, jnp.where(pick == col % 4 * 16 + col // 64 * 4 + v, 1.0, 0.0).astype(F32))
        right = dot(c_mat, jnp.where(pick == v * 4 + col // 16 % 4, 1.0, 0.0).astype(F32))
        total = total + left * right
    krow = lax.broadcasted_iota(jnp.int32, (256, 256), 0)
    kcol = lax.broadcasted_iota(jnp.int32, (256, 256), 1)
    kron[...] = jnp.where(krow // 16 % 4 == kcol // 4 % 4, total, 0.0)
    for cp in env[4:20]:
        cp.wait()
    for fc in range(4):
        for r in range(4):
            t = t1r[3, fc // 2 * 256:(fc // 2 + 1) * 256, (fc % 2 * 4 + r) * LANE:(fc % 2 * 4 + r + 1) * LANE].T
            rt[fc * 2, r * HALF:(r + 1) * HALF, :] = t[:HALF]
            rt[fc * 2 + 1, r * HALF:(r + 1) * HALF, :] = t[HALF:]

    def stage1(fh, ch, g, first, which=range(8)):
        xs = jnp.concatenate([
            jnp.concatenate([xg[fh, g, ch, k, n] for n in which], axis=1) for k in range(2)], axis=0)
        t = dot(l2[ch], xs)
        buf = g if fh == 0 else lax.rem(g + 4, 5)
        for i, n in enumerate(which):
            lanes = slice(i * LANE, (i + 1) * LANE)
            held = pl.ds(n * LANE if isinstance(n, int) else pl.multiple_of(n * LANE, LANE), LANE)
            if first:
                t1r[buf, :, held] = t[:, lanes]
                continue
            for m in range(2):
                v = [t[ab * LANE:(ab + 1) * LANE, lanes] + t1r[buf, ab * LANE:(ab + 1) * LANE, held] for ab in (2 * m, 2 * m + 1)]
                for qb, w in enumerate(swap(*v)):
                    row0 = (2 * n + qb) * 16
                    row0 = row0 if isinstance(n, int) else pl.multiple_of(row0, 16)
                    t1g[:, pl.ds(row0, 16), m * LANE:(m + 1) * LANE] = (w * scale[0:1, 0:1]).reshape(GROUPS, 16, LANE)

    def stage2(g):
        sc = scale[0:1, 0:1]

        def body(_, c):
            for i in range(GROUPS):
                t = dot(kron[...], t1g[i]) * sc
                for rp in range(2):
                    for m in range(2):
                        v = [t[r * HALF:(r + 1) * HALF, m * LANE:(m + 1) * LANE] for r in (2 * rp, 2 * rp + 1)]
                        for n, w in enumerate(swap(*v)):
                            row0 = (2 * m + n) * 512 + i * 64
                            t3s[row0:row0 + 64, rp * LANE:(rp + 1) * LANE] = w
            return c

        lax.fori_loop(g, g + 1, body, 0)

    def stage3(fh, g, final=False):
        def body(i, c):
            rows = pl.ds(i * 1024, 1024) if final else pl.ds(0, 2048)
            part = dot(t3s[rows, :], rt[fh * 4 + g])
            for b in range(2):
                v = part[:, b * LANE:(b + 1) * LANE]
                v = v + (jnp.where(g == 0, 0.0, ys[b, rows]) if fh == 0 else ys[b, rows])
                if final:
                    yo[b, pl.ds(i * 64, 64)] = v.reshape(64, 4, 4, LANE)
                    out_copy(b, i).start()
                else:
                    ys[b] = v
            return c

        if final:
            lax.fori_loop(0, 2, body, 0)
        else:
            lax.fori_loop(g, g + 1, body, 0)

    def out_copy(b, i):
        part = pl.ds(i * 64, 64)
        return pltpu.make_async_copy(yo.at[b, part], y_ref.at[part, :, :, pl.ds(b * LANE, LANE)], out_sem.at[b, i])

    def own(i, _):
        for j in range(2):
            arrived(OWN, OWN, 1 - core, 2 * i + j)
        for j in range(2):
            stage1(OWN, OWN, 2 * i + j, True)
        return 0

    lax.fori_loop(0, 2, own, 0)

    def diagonal(g):
        for half in range(2):
            arrived(OTHER, OTHER, 1 - core, g, half)
        stage1(OTHER, OTHER, g, False)
        stage2(g)

    def direct(g, _):
        @pl.when(g < 3)
        def _():
            relay(g)
            stage1(OWN, OTHER, g, False)
            stage1(OTHER, OWN, g, True)

        def halves(half, c):
            relay_half(g, half)
            which = [4 * half + n for n in range(4)]
            stage1(OWN, OTHER, g, False, which)
            stage1(OTHER, OWN, g, True, which)
            return c

        @pl.when(g == 3)
        def _():
            lax.fori_loop(0, 2, halves, 0)
        stage2(g)
        pl.when(g > 0)(lambda: relay_diag(g - 1))
        stage3(OWN, g)

        @pl.when(g > 0)
        def _():
            diagonal(g - 1)
            pl.when(g == 3)(lambda: relay_diag(g))
            stage3(OTHER, g - 1)

        return 0

    lax.fori_loop(0, 4, direct, 0)

    def rest(g, _):
        diagonal(g)
        stage3(OTHER, g, True)
        return 0

    lax.fori_loop(3, 4, rest, 0)

    for g in range(4):
        for kind in range(7):
            for half in ((None,) if kind == 2 else (0, 1) if kind > 4 else parts(g)):
                send(kind, g, half).wait_send()
    for i in range(2):
        for b in range(2):
            out_copy(b, i).wait()


def solution(mesh):
    def local_apply(x, left, mpo, right):
        any_spec = pl.BlockSpec(memory_space=pl.ANY)
        return pl.pallas_call(
            kernel,
            out_shape=jax.ShapeDtypeStruct((128, 4, 4, 256), F32),
            in_specs=[any_spec] * 4,
            out_specs=any_spec,
            scratch_shapes=[
                pltpu.VMEM((2, 4, 2, 2, 8, 128, LANE), F32),
                pltpu.VMEM((2, 2, 128, 4, LANE), F32),
                pltpu.VMEM((2, 512, 256), F32),
                pltpu.VMEM((8, 256, 256), F32),
                pltpu.VMEM((5, 512, 1024), F32),
                pltpu.VMEM((GROUPS, 256, 256), F32),
                pltpu.VMEM((2048, 256), F32),
                pltpu.VMEM((2, 2048, LANE), F32),
                pltpu.VMEM((2, 128, 4, 4, LANE), F32),
                pltpu.VMEM((256, 256), F32),
                pltpu.SMEM((4, 4, 4, 4), F32),
                pltpu.VMEM((8, LANE), F32),
                pltpu.VMEM((16, LANE), F32),
                pltpu.VMEM((8, LANE), F32),
                pltpu.SemaphoreType.DMA((2, 16)),
                pltpu.SemaphoreType.DMA((21,)),
                pltpu.SemaphoreType.DMA((2, 2)),
                pltpu.SemaphoreType.DMA((7, 4, 2)),
                pltpu.SemaphoreType.DMA((2, 4, 2, 2, 2)),
            ],
            compiler_params=pltpu.CompilerParams(collective_id=0, has_side_effects=True, vmem_limit_bytes=62 * 2**20),
            name='two_site',
        )(x, left, mpo, right)

    return jax.shard_map(local_apply, mesh=mesh, in_specs=(P('bx', None, None, 'by'), P('bx', None, None), P(), P('by', None, None)), out_specs=P('bx', None, None, 'by'), check_vma=False)
```

```python
import functools

import jax
import jax.numpy as jnp
from jax import lax
from jax.experimental import pallas as pl
from jax.experimental.pallas import tpu as pltpu
from jax.sharding import PartitionSpec as P

HI = lax.Precision.HIGHEST
F32 = jnp.float32
LANE = 128
HALF = 64
GROUPS = 8
OWN, OTHER = 0, 1


def dot(a, b):
    return jnp.dot(a, b, precision=HI, preferred_element_type=F32)


def kernel(x_ref, l_ref, w_hbm, r_ref, y_ref, xg, ln, l2, rt, t1r, t1g, t3s, ys, yo, kron, w_ref, wa, wb, scale, load_sem, env_sem, out_sem, send_sem, recv_sem):
    by = lax.axis_index('by')
    bx = lax.axis_index('bx')
    core = lax.rem(bx, 2)
    chip = bx // 2
    sib = {'by': by, 'bx': bx + 1 - 2 * core}
    xnb = {'by': by, 'bx': lax.rem(bx + 2, 4)}
    ynb = {'by': 1 - by, 'bx': bx}

    def load(h, pq):
        i = h * 16 + pq
        return pltpu.make_async_copy(
            x_ref.at[:, pq // 4, pq % 4, pl.ds(h * LANE, LANE)],
            t1r.at[4, pl.ds(i // 8 * LANE, LANE), pl.ds(i % 8 * LANE, LANE)], load_sem.at[h, pq])

    for h in range(2):
        for pq in range(16):
            load(h, pq).start()
    barrier = pltpu.get_barrier_semaphore()
    for d in (sib, xnb, ynb):
        pl.semaphore_signal(barrier, inc=1, device_id=d, device_id_type=pl.DeviceIdType.MESH)
    def send(kind, g, half):
        fh, ch = ((0, 0), (0, 0), (0, 0), (0, 1), (1, 0), (1, 1), (half, 1 - half))[kind]
        dh, dc = ((0, 1), (1, 0), (0, 0), (0, 1), (1, 0), (1, 1), (1, 1))[kind]
        to = (xnb, ynb, sib, sib, sib, sib, (ynb, xnb)[half])[kind]
        return pltpu.make_async_remote_copy(
            src_ref=xg.at[fh, g, ch, core, pl.ds(4 * half, 4)],
            dst_ref=xg.at[dh, g, dc, core, pl.ds(4 * half, 4)],
            send_sem=send_sem.at[kind, g, half],
            recv_sem=recv_sem.at[dh, g, dc, core, half],
            device_id=to, device_id_type=pl.DeviceIdType.MESH)

    def arrived(fh, ch, k, g, half):
        ref = xg.at[fh, g, ch, k, pl.ds(4 * half, 4)]
        pltpu.make_async_copy(ref, ref, recv_sem.at[fh, g, ch, k, half]).wait()

    def all_arrived(fh, ch, g):
        for half in range(2):
            arrived(fh, ch, 1 - core, g, half)

    def direct_sends(g):
        for half in range(2):
            send(0, g, half).start()
            send(1, g, half).start()

    low = lax.broadcasted_iota(jnp.int32, (LANE, LANE), 1) < HALF

    def swap(v0, v1):
        m = low[:v0.shape[0]]
        return jnp.where(m, v0, pltpu.roll(v1, HALF, 1)), jnp.where(m, pltpu.roll(v0, HALF, 1), v1)

    def split(h, half):
        for pq in range(8 * half, 8 * half + 8):
            load(h, pq).wait()
        for n in range(4 * half, 4 * half + 4):
            blocks = [(h * 16 + pq) for pq in (2 * n, 2 * n + 1)]
            v = [t1r[4, i // 8 * LANE:(i // 8 + 1) * LANE, i % 8 * LANE:(i % 8 + 1) * LANE] for i in blocks]
            xg[OWN, 2 * h, OWN, core, n], xg[OWN, 2 * h + 1, OWN, core, n] = swap(*v)

    split(0, 0)
    pl.semaphore_wait(barrier, 3)
    for half in range(2):
        if half == 1:
            split(0, 1)
        for kind in range(2):
            send(kind, 0, half).start()
    direct_sends(1)
    for g in range(2):
        for half in range(2):
            send(2, g, half).start()
    env = []
    for half in range(2):
        for k in range(2):
            c0 = ((chip + half) % 2 * 2 + k) * LANE
            env.append(pltpu.make_async_copy(
                l_ref.at[:, :, pl.ds(pl.multiple_of(c0, LANE), LANE)], ln.at[half, k], env_sem.at[half * 2 + k]))
    for half in range(2):
        for h in range(2):
            f0 = ((by + half) % 2 * 2 + h) * LANE
            for r in range(4):
                env.append(pltpu.make_async_copy(
                    r_ref.at[:, r, pl.ds(pl.multiple_of(f0, LANE), LANE)],
                    t1r.at[3, pl.ds(half * 256, 256), pl.ds((h * 4 + r) * LANE, LANE)],
                    env_sem.at[4 + (half * 2 + h) * 4 + r]))
    env.append(pltpu.make_async_copy(w_hbm, w_ref, env_sem.at[20]))
    for cp in env:
        cp.start()


    split(1, 0)
    split(1, 1)
    for g in range(2, 4):
        for half in range(2):
            send(2, g, half).start()

    def relay(g):
        for half in range(2):
            arrived(OWN, OTHER, core, g, half)
            send(3, g, half).start()
            if half == 0:
                send(6, g, half).start()
            arrived(OTHER, OWN, core, g, half)
            send(4, g, half).start()
            if half == 1:
                send(6, g, half).start()
        pl.when(g < 2)(lambda: direct_sends(g + 2))

    def relay_diag(g):
        for half in range(2):
            arrived(OTHER, OTHER, core, g, half)
            send(5, g, half).start()

    for cp in env[:4] + env[20:]:
        cp.wait()
    for half in range(2):
        for k in range(2):
            l2[half, :, k * LANE:(k + 1) * LANE] = ln[half, k].reshape(512, LANE)
    wa[...] = jnp.zeros_like(wa)
    wb[...] = jnp.zeros_like(wb)
    lane8 = lax.broadcasted_iota(jnp.int32, (8, LANE), 1)
    row8 = lax.broadcasted_iota(jnp.int32, (8, LANE), 0)
    lane16 = lax.broadcasted_iota(jnp.int32, (16, LANE), 1)
    row16 = lax.broadcasted_iota(jnp.int32, (16, LANE), 0)

    def fill(i, carry):
        va, vb = carry
        i0, i1, i2 = i // 16, i // 4 % 4, i % 4
        for i3 in range(4):
            val = w_ref[i0, i1, i2, i3]
            va = jnp.where((row8 == i1) & (lane8 == i0 * 16 + i2 * 4 + i3), val, va)
            vb = jnp.where((row16 == i3 * 4 + i1) & (lane16 == i0 * 4 + i2), val, vb)
        return va, vb

    va, vb = lax.fori_loop(0, 64, fill, (jnp.zeros((8, LANE), F32), jnp.zeros((16, LANE), F32)), unroll=4)
    top = jnp.max(jnp.max(jnp.abs(va), axis=1, keepdims=True), axis=0, keepdims=True)
    scale[...] = jnp.broadcast_to(top, scale.shape)
    wa[...] = va / scale[...]
    wb[...] = vb / jnp.broadcast_to(top, (16, LANE))

    row = lax.broadcasted_iota(jnp.int32, (256, LANE), 0)
    a_mat = jnp.zeros((256, LANE), F32)
    for s in range(4):
        a_mat = jnp.where(row // 4 % 4 == s, wa[s:s + 1, :], a_mat)
    c_mat = jnp.zeros((256, LANE), F32)
    for rt_ in range(16):
        c_mat = jnp.where((row // 64) * 4 + row % 4 == rt_, wb[rt_:rt_ + 1, :], c_mat)
    col = lax.broadcasted_iota(jnp.int32, (LANE, 256), 1)
    pick = lax.broadcasted_iota(jnp.int32, (LANE, 256), 0)
    total = jnp.zeros((256, 256), F32)
    for v in range(4):
        left = dot(a_mat, jnp.where(pick == col % 4 * 16 + col // 64 * 4 + v, 1.0, 0.0).astype(F32))
        right = dot(c_mat, jnp.where(pick == v * 4 + col // 16 % 4, 1.0, 0.0).astype(F32))
        total = total + left * right
    krow = lax.broadcasted_iota(jnp.int32, (256, 256), 0)
    kcol = lax.broadcasted_iota(jnp.int32, (256, 256), 1)
    kron[...] = jnp.where(krow // 16 % 4 == kcol // 4 % 4, total, 0.0)
    for cp in env[4:20]:
        cp.wait()
    for fc in range(4):
        for r in range(4):
            t = t1r[3, fc // 2 * 256:(fc // 2 + 1) * 256, (fc % 2 * 4 + r) * LANE:(fc % 2 * 4 + r + 1) * LANE].T
            rt[fc * 2, r * HALF:(r + 1) * HALF, :] = t[:HALF]
            rt[fc * 2 + 1, r * HALF:(r + 1) * HALF, :] = t[HALF:]

    def stage1(fh, ch, g, first):
        xs = jnp.concatenate([
            jnp.concatenate([xg[fh, g, ch, k, n] for n in range(8)], axis=1) for k in range(2)], axis=0)
        t = dot(l2[ch], xs)
        buf = g if fh == 0 else lax.rem(g + 4, 5)
        if first:
            t1r[buf] = t
            return
        for n in range(8):
            lanes = slice(n * LANE, (n + 1) * LANE)
            for m in range(2):
                v = [t[ab * LANE:(ab + 1) * LANE, lanes] + t1r[buf, ab * LANE:(ab + 1) * LANE, lanes] for ab in (2 * m, 2 * m + 1)]
                for qb, w in enumerate(swap(*v)):
                    t1g[:, (2 * n + qb) * 16:(2 * n + qb + 1) * 16, m * LANE:(m + 1) * LANE] = (w * scale[0:1, 0:1]).reshape(GROUPS, 16, LANE)

    def stage2(g):
        sc = scale[0:1, 0:1]

        def body(_, c):
            for i in range(GROUPS):
                t = dot(kron[...], t1g[i]) * sc
                for rp in range(2):
                    for m in range(2):
                        v = [t[r * HALF:(r + 1) * HALF, m * LANE:(m + 1) * LANE] for r in (2 * rp, 2 * rp + 1)]
                        for n, w in enumerate(swap(*v)):
                            row0 = (2 * m + n) * 512 + i * 64
                            t3s[row0:row0 + 64, rp * LANE:(rp + 1) * LANE] = w
            return c

        lax.fori_loop(g, g + 1, body, 0)

    def stage3(fh, g, final=False):
        def body(i, c):
            rows = pl.ds(i * 1024, 1024) if final else pl.ds(0, 2048)
            part = dot(t3s[rows, :], rt[fh * 4 + g])
            for b in range(2):
                v = part[:, b * LANE:(b + 1) * LANE]
                v = v + (jnp.where(g == 0, 0.0, ys[b, rows]) if fh == 0 else ys[b, rows])
                if final:
                    yo[b, pl.ds(i * 64, 64)] = v.reshape(64, 4, 4, LANE)
                    out_copy(b, i).start()
                else:
                    ys[b] = v
            return c

        if final:
            lax.fori_loop(0, 2, body, 0)
        else:
            lax.fori_loop(g, g + 1, body, 0)

    def out_copy(b, i):
        part = pl.ds(i * 64, 64)
        return pltpu.make_async_copy(yo.at[b, part], y_ref.at[part, :, :, pl.ds(b * LANE, LANE)], out_sem.at[b, i])

    def own(i, _):
        for j in range(2):
            all_arrived(OWN, OWN, 2 * i + j)
        for j in range(2):
            stage1(OWN, OWN, 2 * i + j, True)
        return 0

    lax.fori_loop(0, 2, own, 0)

    def diagonal(g):
        all_arrived(OTHER, OTHER, g)
        stage1(OTHER, OTHER, g, False)
        stage2(g)

    def direct(g, _):
        relay(g)
        all_arrived(OWN, OTHER, g)
        all_arrived(OTHER, OWN, g)
        stage1(OWN, OTHER, g, False)
        stage1(OTHER, OWN, g, True)
        stage2(g)
        pl.when(g > 0)(lambda: relay_diag(g - 1))
        stage3(OWN, g)

        @pl.when(g > 0)
        def _():
            diagonal(g - 1)
            pl.when(g == 3)(lambda: relay_diag(g))
            stage3(OTHER, g - 1)

        return 0

    lax.fori_loop(0, 4, direct, 0)

    def rest(g, _):
        diagonal(g)
        stage3(OTHER, g, True)
        return 0

    lax.fori_loop(3, 4, rest, 0)

    for kind in range(7):
        for g in range(4):
            for half in range(2):
                send(kind, g, half).wait_send()
    for i in range(2):
        for b in range(2):
            out_copy(b, i).wait()


def solution(mesh):
    def local_apply(x, left, mpo, right):
        any_spec = pl.BlockSpec(memory_space=pl.ANY)
        return pl.pallas_call(
            kernel,
            out_shape=jax.ShapeDtypeStruct((128, 4, 4, 256), F32),
            in_specs=[any_spec] * 4,
            out_specs=any_spec,
            scratch_shapes=[
                pltpu.VMEM((2, 4, 2, 2, 8, 128, LANE), F32),
                pltpu.VMEM((2, 2, 128, 4, LANE), F32),
                pltpu.VMEM((2, 512, 256), F32),
                pltpu.VMEM((8, 256, 256), F32),
                pltpu.VMEM((5, 512, 1024), F32),
                pltpu.VMEM((GROUPS, 256, 256), F32),
                pltpu.VMEM((2048, 256), F32),
                pltpu.VMEM((2, 2048, LANE), F32),
                pltpu.VMEM((2, 128, 4, 4, LANE), F32),
                pltpu.VMEM((256, 256), F32),
                pltpu.SMEM((4, 4, 4, 4), F32),
                pltpu.VMEM((8, LANE), F32),
                pltpu.VMEM((16, LANE), F32),
                pltpu.VMEM((8, LANE), F32),
                pltpu.SemaphoreType.DMA((2, 16)),
                pltpu.SemaphoreType.DMA((21,)),
                pltpu.SemaphoreType.DMA((2, 2)),
                pltpu.SemaphoreType.DMA((7, 4, 2)),
                pltpu.SemaphoreType.DMA((2, 4, 2, 2, 2)),
            ],
            compiler_params=pltpu.CompilerParams(collective_id=0, has_side_effects=True, vmem_limit_bytes=62 * 2**20),
            name='two_site',
        )(x, left, mpo, right)

    return jax.shard_map(local_apply, mesh=mesh, in_specs=(P('bx', None, None, 'by'), P('bx', None, None), P(), P('by', None, None)), out_specs=P('bx', None, None, 'by'), check_vma=False)
```
